128 devices in a mesh: node: 8 (over z_hi, x), row: 16 (over y, z_lo, core).
Axes of the slice: x: 4, y: 4, z: 4 (z_hi: 2, z_lo: 2; z = z_hi * 2 + z_lo), core: 2. Of those that a mesh axis runs over, the one named last changes fastest.
Arguments:
- inputs: float32 [16, 64, 128, 128], P(None, 'row'), may hold values from -8 to 8
- diagonal: float32 [64, 128, 128], P('row'), may hold values from 0.05 to 1
- observations: float32 [16, 64, 128, 128], P(None, 'row'), may hold values from -0.005859375 to 0.005859375
- frequencies: float32 [8], replicated, may hold values from 0.2 to 3
- weights: float32 [8], replicated, may hold values from 0.5 to 2
- counts: int32 [8], replicated, may hold values from 3 to 6, as said below
- assignment: int32 [8], replicated, may hold values from 0 to 7, each once
Outputs:
- probe_response: float32 [16, 64, 128, 128], P(None, 'row')
- group_gram: float32 [8, 16, 16], P('node')
The draws below stay inside these ranges and needn't reach their ends.
Inputs may be any that keep to these rules, and one draw needn't show every extreme that they name: `counts`: some node has 6 sweeps and some node 3 in every draw. `assignment`: each node 0 to 7 appears once.
All inputs are finite; a program needn't handle non-finite values.
Results may differ from the reference program's by a relative error of at most 0.0003.
Values sent between devices are 32-bit elements; how exact they have to be, the bound alone decides.
No kernel may reach another device: no remote copies, remote signals or barrier semaphores. Data moves between devices by JAX's collectives and lax.ppermute only.
A program may use at most 192 MiB of HBM per device.

```python
import math
import jax
import jax.numpy as jnp
from jax import lax

INPUTS = 16
PROBES = 16
GY = 128
GZ = 128
NODE_DEV = 1
ITERS = 6
QUAD = 8
NX = 64
CELLS = 1048576
N_NODE = 8


def draw_inputs(key, part):
    values = jnp.clip(2.0 * jax.random.normal(key, (INPUTS, NX, GY, GZ), jnp.float32), -8.0, 8.0)
    return values.astype(jnp.float32)


def draw_counts(key, part):
    first, second, third = jax.random.split(jax.random.fold_in(key, 17), 3)
    values = jax.random.randint(first, (QUAD,), ITERS // 2, ITERS + 1, jnp.int32)
    top_slot = jax.random.randint(second, (), 0, QUAD, jnp.int32)
    low_slot = (top_slot + 1 + jax.random.randint(third, (), 0, QUAD - 1, jnp.int32)) % QUAD
    values = values.at[top_slot].set(ITERS)
    values = values.at[low_slot].set(ITERS // 2)
    return values.astype(jnp.int32)


def block_scale(stream_key, extent, cuts, least, high):
    gain, own = 1.0, jax.random.fold_in(stream_key, 6)
    for position, blocks in cuts:
        heights = jnp.exp(jax.random.uniform(jax.random.fold_in(own, position), (blocks,), jnp.float32, least / len(cuts), high / len(cuts)))
        gain = gain * jnp.repeat(heights, extent[position] // blocks).reshape([-1 if axis == position else 1 for axis in range(len(extent))])
    return gain


def normal_values(own_key, shape, width, bound, pieces=(), kind=jnp.bfloat16):
    entries = jax.random.normal(own_key, shape, jnp.float32) * width
    if len(pieces) > 0:
        entries = block_scale(own_key, shape, pieces, -0.22, 0.18) * entries
    return jnp.clip(entries, min=-bound, max=bound).astype(kind)


def setup_inputs(seed: int = 0) -> dict:
    seeds = jax.random.split(jax.random.key(seed), 8)
    inputs = draw_inputs(jax.random.fold_in(seeds[7], 71), 0)
    diagonal = jnp.clip(jnp.exp(math.log(1.0) - 2.9957323 * jax.random.uniform(seeds[1], (NX, GY, GZ), jnp.float32) ** block_scale(seeds[1], (NX, GY, GZ), ((0, 16),), -0.2, 0.2)), 0.05, 1.0)
    observations = normal_values(seeds[2], (PROBES, NX, GY, GZ), CELLS ** -0.5, 0.005859375, ((1, 16),), jnp.float32)
    frequencies = jnp.clip(jax.random.uniform(seeds[3], (QUAD,), jnp.float32, 0.2, 3.0), 0.2, 3.0)
    weights = jnp.clip(jnp.exp(jax.random.uniform(seeds[4], (QUAD,), jnp.float32, math.log(0.5), math.log(2.0))), 0.5, 2.0)
    counts = draw_counts(jax.random.fold_in(seeds[7], 71), 0)
    assignment = jax.random.permutation(seeds[6], QUAD).astype(jnp.int32)
    return {"inputs": inputs, "diagonal": diagonal, "observations": observations, "frequencies": frequencies, "weights": weights, "counts": counts, "assignment": assignment}


def relax_step(fields, source, diagonal, shift_val, active):
    padded = jnp.pad(fields, ((0, 0), (0, 0), (1, 1), (1, 1), (1, 1)))
    beside = padded[:, :, 2:, 1:-1, 1:-1] + padded[:, :, :-2, 1:-1, 1:-1]
    beside = beside + padded[:, :, 1:-1, 2:, 1:-1] + padded[:, :, 1:-1, :-2, 1:-1]
    beside = beside + padded[:, :, 1:-1, 1:-1, 2:] + padded[:, :, 1:-1, 1:-1, :-2]
    diag_full = 6.0 + diagonal
    applied = diag_full * fields - beside
    resid_real = source - applied[0] + shift_val * fields[1]
    resid_imag = -applied[1] - shift_val * fields[0]
    denominator = diag_full * diag_full + shift_val * shift_val
    step_real = (diag_full * resid_real + shift_val * resid_imag) / denominator
    step_imag = (diag_full * resid_imag - shift_val * resid_real) / denominator
    return fields + active * jnp.stack([step_real, step_imag], 0)


def reference(inputs, diagonal, observations, frequencies, weights, counts, assignment):
    cells = NX * GY * GZ
    flat_probe = observations.reshape(PROBES, cells)

    def one_node(carry, node_id):
        shift_val = frequencies[node_id]
        fields = jnp.zeros((2,) + inputs.shape, jnp.float32)
        for sweep in range(ITERS):
            active = (sweep < counts[node_id]).astype(jnp.float32)
            fields = relax_step(fields, inputs, diagonal, shift_val, active)
        flat_fields = fields.reshape(2, INPUTS, cells)
        projected = jnp.einsum("aic,pc->aip", flat_fields, flat_probe, precision=lax.Precision.HIGHEST)
        gram_part = jnp.einsum("aic,ajc->ij", flat_fields, flat_fields, precision=lax.Precision.HIGHEST)
        contrib = jnp.einsum("aip,aic->pc", projected, flat_fields, precision=lax.Precision.HIGHEST)
        return carry + weights[node_id] * contrib, weights[node_id] * gram_part

    start = jnp.zeros((PROBES, cells), jnp.float32)
    total, grams = lax.scan(one_node, start, jnp.arange(QUAD, dtype=jnp.int32))
    probe_response = (total / QUAD).reshape(PROBES, NX, GY, GZ)
    group_gram = grams[assignment].reshape(N_NODE, NODE_DEV, INPUTS, INPUTS).sum(1) / cells
    return probe_response, group_gram
```

```python
import jax
import jax.numpy as jnp
from jax import lax
from jax.experimental import pallas as pl
from jax.experimental.pallas import tpu as pltpu
from jax.sharding import PartitionSpec as P

QUAD = 8
COLS = 16
DEPTH = 5
PLANES = 4
ROWS = 16
WIDE = ROWS + 2 * DEPTH
SPAN = PLANES + 2 * DEPTH
LANES = 128
CELLS = 1048576.0
SEND_B = sum(WIDE - 2 * d for d in range(1, PLANES + 1)) * COLS
SEND_E = PLANES * 24
FAR_B = ROWS * COLS
OWN_B = PLANES * WIDE * COLS
F32 = jnp.float32
BF16 = jnp.bfloat16
VMEM = pl.BlockSpec(memory_space=pltpu.VMEM)
SMEM = pl.BlockSpec(memory_space=pltpu.SMEM)
ANY = pl.BlockSpec(memory_space=pl.ANY)


def pack_kernel(at_ref, src_ref, diag_ref, own_ref, fwd_ref, bwd_ref, fwd2_ref, bwd2_ref, edge_ref):
    edge_ref[...] = jnp.zeros_like(edge_ref)
    for x in range(PLANES):
        edge_ref[x, pl.ds(16, 128), :] = diag_ref[x] + 6.0

    def rows(dst_ref, base, plane, first, count):
        for q in range(count):
            y = jnp.clip(first + q, 0, 127)
            dst_ref[pl.ds(base + q * COLS, COLS), :] = src_ref[
                pl.ds(plane * 128 + y, COLS, stride=PLANES * 128), :
            ]

    own = at_ref[0]
    for x in range(PLANES):
        rows(own_ref, x * WIDE * COLS, x, own - DEPTH, WIDE)
        own_ref[pl.ds(OWN_B + x * 32, 32), :] = edge_ref[x, pl.ds(16 + own - DEPTH, 32), :]
    base = 0
    for d in range(1, PLANES + 1):
        count = WIDE - 2 * d
        for dst_ref, at, plane in ((fwd_ref, at_ref[1], PLANES - d), (bwd_ref, at_ref[2], d - 1)):
            rows(dst_ref, base, plane, at - DEPTH + d, count)
            dst_ref[pl.ds(SEND_B + (d - 1) * 24, 24), :] = edge_ref[
                plane, pl.ds(16 + at - DEPTH + d, 24), :
            ]
        base += count * COLS
    for dst_ref, at, plane in ((fwd2_ref, at_ref[3], PLANES - 1), (bwd2_ref, at_ref[4], 0)):
        rows(dst_ref, 0, plane, at, ROWS)
        dst_ref[pl.ds(FAR_B, ROWS), :] = edge_ref[plane, pl.ds(16 + at, ROWS), :]


def pack(at, inputs, diagonal):
    out = lambda n: jax.ShapeDtypeStruct((n, LANES), F32)
    return pl.pallas_call(
        pack_kernel,
        out_shape=(
            out(OWN_B + PLANES * 32),
            out(SEND_B + SEND_E),
            out(SEND_B + SEND_E),
            out(FAR_B + ROWS),
            out(FAR_B + ROWS),
        ),
        in_specs=[SMEM, VMEM, VMEM],
        out_specs=(VMEM,) * 5,
        scratch_shapes=[pltpu.VMEM((PLANES, 160, LANES), F32)],
        compiler_params=pltpu.CompilerParams(vmem_limit_bytes=24 << 20),
        name="pack",
    )(at, inputs.reshape(COLS * PLANES * 128, LANES), diagonal)


def solve_kernel(
    at_ref, freq_ref, count_ref, own_ref, low_ref, high_ref, low2_ref, high2_ref, obs_ref,
    hi_ref, lo_ref, part_ref,
    src, field, edge, gre, gim, cat, obs, stage, sems,
):
    node = pl.program_id(0)

    @pl.when(node == 0)
    def _():
        copies = []

        def fetch(a, b):
            copies.append(pltpu.make_async_copy(a, b, sems.at[len(copies)]))
            copies[-1].start()

        fetch(obs_ref.at[:, :, pl.ds(pl.multiple_of(at_ref[0], 16), ROWS), :], obs)
        for x in range(PLANES):
            fetch(
                own_ref.at[pl.ds(x * WIDE * COLS, WIDE * COLS)],
                src.at[DEPTH + x],
            )
        fetch(own_ref.at[pl.ds(OWN_B, PLANES * 32)], stage.at[pl.ds(0, 128)])
        for s, (near, far) in enumerate(((low_ref, low2_ref), (high_ref, high2_ref))):
            base = 0
            for d in range(1, PLANES + 1):
                count = (WIDE - 2 * d) * COLS
                px = DEPTH - d if s == 0 else DEPTH + PLANES - 1 + d
                fetch(near.at[pl.ds(base, count)], src.at[px, pl.ds(d * COLS, count)])
                base += count
            px = 0 if s == 0 else SPAN - 1
            fetch(far.at[pl.ds(0, FAR_B)], src.at[px, pl.ds(DEPTH * COLS, FAR_B)])
            fetch(near.at[pl.ds(SEND_B, SEND_E)], stage.at[pl.ds(128 + s * 112, SEND_E)])
            fetch(far.at[pl.ds(FAR_B, ROWS)], stage.at[pl.ds(128 + s * 112 + 96, ROWS)])
        edge[...] = jnp.zeros_like(edge)
        part_ref[...] = jnp.zeros_like(part_ref)
        cat[96:128, :] = jnp.zeros((32, PLANES * ROWS * LANES), BF16)
        for c in copies:
            c.wait()
        for x in range(PLANES):
            edge[DEPTH + x] = stage[pl.ds(x * 32, 32), :]
            for y in range(ROWS):
                v = obs[:, x, y, :]
                hi = v.astype(BF16)
                at = pl.ds((x * ROWS + y) * LANES, LANES)
                cat[64:80, at] = hi
                cat[80:96, at] = (v - hi.astype(F32)).astype(BF16)
        for s in range(2):
            for d in range(1, DEPTH + 1):
                px = DEPTH - d if s == 0 else DEPTH + PLANES - 1 + d
                edge[px, pl.ds(d, WIDE - 2 * d), :] = stage[
                    pl.ds(128 + s * 112 + (d - 1) * 24, WIDE - 2 * d), :
                ]

    count = count_ref[node]
    freq = freq_ref[node]

    @pl.loop(0, SPAN)
    def _(px):
        d = edge[px]
        inv = 1.0 / (d * d + freq * freq)
        gre[px] = d * inv
        gim[px] = jnp.where(d > 0.0, freq * inv, 0.0)

    def planes(level, m, body):
        dd = level - m
        trips = jnp.where(dd < 0, 0, jnp.where(dd == 0, PLANES, 2))

        @pl.loop(0, trips)
        def _(q):
            px = jnp.where(
                dd == 0, DEPTH + q, jnp.where(q == 0, DEPTH - dd, DEPTH + PLANES - 1 + dd)
            )
            body(px)

    def spread(ref, px, r):
        return jnp.broadcast_to(ref[px, pl.ds(r, 1), :], (COLS, LANES))

    level0 = count - 1
    par0 = lax.rem(level0, 2)
    for m in range(DEPTH + 1):

        def first(px, m=m):
            for r in range(DEPTH - m, DEPTH + ROWS + m):
                b = src[px, pl.ds(r * COLS, COLS), :]
                field[par0, 0, px, pl.ds(r * COLS, COLS), :] = spread(gre, px, r) * b
                field[par0, 1, px, pl.ds(r * COLS, COLS), :] = -(spread(gim, px, r) * b)

        planes(level0, m, first)

    lane = lax.broadcasted_iota(jnp.int32, (COLS, LANES), 1)
    not_first = lane > 0
    not_last = lane < LANES - 1

    def beside(v):
        return jnp.where(not_first, pltpu.roll(v, 1, 1), 0.0) + jnp.where(
            not_last, pltpu.roll(v, LANES - 1, 1), 0.0
        )

    @pl.loop(0, count - 1)
    def _(t):
        level = count - 2 - t
        new = lax.rem(level, 2)
        old = 1 - new
        for m in range(DEPTH):

            def sweep(px, m=m):
                def get(c, p, r):
                    return field[old, c, p, pl.ds(r * COLS, COLS), :]

                start = DEPTH - m
                below = [get(c, px, start - 1) for c in range(2)]
                here = [get(c, px, start) for c in range(2)]
                for r in range(start, DEPTH + ROWS + m):
                    above = [get(c, px, r + 1) for c in range(2)]
                    total = [
                        (get(c, px - 1, r) + get(c, px + 1, r))
                        + (below[c] + above[c])
                        + beside(here[c])
                        for c in range(2)
                    ]
                    a = total[0] + src[px, pl.ds(r * COLS, COLS), :]
                    b = total[1]
                    p, q = spread(gre, px, r), spread(gim, px, r)
                    field[new, 0, px, pl.ds(r * COLS, COLS), :] = p * a + q * b
                    field[new, 1, px, pl.ds(r * COLS, COLS), :] = p * b - q * a
                    below, here = here, above

            planes(level, m, sweep)

    @pl.loop(0, PLANES)
    def _(x):
        for y in range(ROWS):
            at = pl.ds(pl.multiple_of(x * (ROWS * LANES) + y * LANES, LANES), LANES)
            for c in range(2):
                v = field[0, c, DEPTH + x, pl.ds((DEPTH + y) * COLS, COLS), :]
                hi = v.astype(BF16)
                lo = (v - hi.astype(F32)).astype(BF16)
                cat[pl.ds(c * COLS, COLS), at] = hi
                cat[pl.ds(32 + c * COLS, COLS), at] = lo
                hi_ref[pl.ds(c * COLS, COLS), at] = hi
                lo_ref[pl.ds(c * COLS, COLS), at] = lo

    o = lax.dot_general(
        cat[0:64, :], cat[...], (((1,), (1,)), ((), ())), preferred_element_type=F32
    )
    wide = lax.broadcasted_iota(jnp.int32, (32, LANES), 1)
    proj = o[0:32] + pltpu.roll(o[0:32], LANES - 16, 1) + o[32:64]
    proj = jnp.where((wide >= 64) & (wide < 80), proj, 0.0)
    part_ref[0:32, :] += pltpu.roll(proj, lax.rem(64 + 16 * node, 128), 1)
    gu = o[0:16] + pltpu.roll(o[0:16], LANES - 32, 1) + o[32:48]
    gw = o[16:32] + pltpu.roll(o[16:32], LANES - 32, 1) + o[48:64]
    gram = jnp.where(lane < 16, gu + pltpu.roll(gw, LANES - 16, 1), 0.0)
    part_ref[32:48, :] += pltpu.roll(gram, 16 * node, 1)


def solve(at, freqs, counts, own, low, high, low2, high2, obs):
    cells = PLANES * ROWS * LANES
    return pl.pallas_call(
        solve_kernel,
        grid=(QUAD,),
        out_shape=(
            jax.ShapeDtypeStruct((QUAD * 32, cells), BF16),
            jax.ShapeDtypeStruct((QUAD * 32, cells), BF16),
            jax.ShapeDtypeStruct((48, LANES), F32),
        ),
        in_specs=[SMEM, SMEM, SMEM] + [ANY] * 6,
        out_specs=(
            pl.BlockSpec((32, cells), lambda k: (k, 0)),
            pl.BlockSpec((32, cells), lambda k: (k, 0)),
            pl.BlockSpec((48, LANES), lambda k: (0, 0)),
        ),
        scratch_shapes=[
            pltpu.VMEM((SPAN, WIDE * COLS, LANES), F32),
            pltpu.VMEM((2, 2, SPAN, WIDE * COLS, LANES), F32),
            pltpu.VMEM((SPAN, 32, LANES), F32),
            pltpu.VMEM((SPAN, 32, LANES), F32),
            pltpu.VMEM((SPAN, 32, LANES), F32),
            pltpu.VMEM((128, cells), BF16),
            pltpu.VMEM((COLS, PLANES, ROWS, LANES), F32),
            pltpu.VMEM((352, LANES), F32),
            pltpu.SemaphoreType.DMA((24,)),
        ],
        compiler_params=pltpu.CompilerParams(
            dimension_semantics=("arbitrary",), vmem_limit_bytes=40 << 20
        ),
        name="solve",
    )(at, freqs, counts, own, low, high, low2, high2, obs)


def respond_kernel(pick_ref, weight_ref, sum_ref, hi_ref, lo_ref, out_ref, gram_ref, coef):
    @pl.when(pl.program_id(0) == 0)
    def _():
        turned = sum_ref[0:32, :].T
        for half in range(2):
            acc = jnp.zeros((16, LANES), F32)
            for j in range(4):
                k = half * 4 + j
                piece = turned[16 * k : 16 * k + 16, :] * (weight_ref[k] * (1.0 / QUAD))
                piece = jnp.concatenate([piece, jnp.zeros((16, 96), F32)], 1)
                acc = acc + (pltpu.roll(piece, 32 * j, 1) if j else piece)
            at = pl.ds(half * LANES, LANES)
            hi = acc.astype(BF16)
            coef[0:16, at] = hi
            coef[16:32, at] = (acc - hi.astype(F32)).astype(BF16)
        node = pick_ref[0]
        gram = pltpu.roll(sum_ref[32:48, :], lax.rem(128 - 16 * node, 128), 1)
        gram_ref[...] = gram * (weight_ref[node] * (1.0 / CELLS))

    big = jnp.dot(coef[...], hi_ref[...], preferred_element_type=F32)
    small = jnp.dot(coef[0:16, :], lo_ref[...], preferred_element_type=F32)
    res = big[0:16] + big[16:32] + small
    for y in range(ROWS):
        out_ref[:, 0, y, :] = res[:, y * LANES : (y + 1) * LANES]


def respond(pick, weights, total, hi, lo):
    wide = ROWS * LANES
    return pl.pallas_call(
        respond_kernel,
        grid=(PLANES,),
        out_shape=(
            jax.ShapeDtypeStruct((16, PLANES, ROWS, LANES), F32),
            jax.ShapeDtypeStruct((16, LANES), F32),
        ),
        in_specs=[
            SMEM,
            SMEM,
            pl.BlockSpec((48, LANES), lambda x: (0, 0)),
            pl.BlockSpec((QUAD * 32, wide), lambda x: (0, x)),
            pl.BlockSpec((QUAD * 32, wide), lambda x: (0, x)),
        ],
        out_specs=(
            pl.BlockSpec((16, 1, ROWS, LANES), lambda x: (0, x, 0, 0)),
            pl.BlockSpec((16, LANES), lambda x: (0, 0)),
        ),
        scratch_shapes=[pltpu.VMEM((32, QUAD * 32), BF16)],
        compiler_params=pltpu.CompilerParams(
            dimension_semantics=("arbitrary",), vmem_limit_bytes=24 << 20
        ),
        name="respond",
    )(pick, weights, total, hi, lo)


def step_pairs(step):
    pairs = []
    for node in range(8):
        for r in range(16):
            t = r + step
            if 0 <= t < 16:
                c, ct = r // 2, t // 2
                flip = c != ct and (c % 2 == 1 if step > 0 else c % 2 == 0)
                pairs.append((node * 16 + r, (node ^ 4 if flip else node) * 16 + t))
    return pairs


def xor_sum(x, axis, size, masks):
    combos = [0]
    for m in masks:
        combos += [c ^ m for c in combos]
    got = [x if c == 0 else lax.ppermute(x, axis, [(i, i ^ c) for i in range(size)]) for c in combos]
    while len(got) > 1:
        got = [got[i] + got[i + 1] for i in range(0, len(got), 2)]
    return got[0]


def turn(v, by):
    return lax.ppermute(v, "node", [(i, i // 4 * 4 + (i + by) % 4) for i in range(8)])


def local(inputs, diagonal, observations, frequencies, weights, counts, assignment):
    node = lax.axis_index("node")
    row = lax.axis_index("row")
    core, odd = row % 2, (row // 2) % 2
    fwd2 = node ^ (4 * odd)
    bwd2 = node ^ (4 * (1 - odd))
    fwd = jnp.where(core == 1, fwd2, node)
    bwd = jnp.where(core == 0, bwd2, node)
    at = (16 * jnp.stack([node, fwd, bwd, fwd2, bwd2])).astype(jnp.int32)
    own, s1, s2, s3, s4 = pack(at, inputs, diagonal)
    both = ("node", "row")
    low = lax.ppermute(s1, both, step_pairs(1))
    high = lax.ppermute(s2, both, step_pairs(-1))
    low2 = lax.ppermute(s3, both, step_pairs(2))
    high2 = lax.ppermute(s4, both, step_pairs(-2))
    hi, lo, part = solve(at, frequencies, counts, own, low, high, low2, high2, observations)
    total = xor_sum(part, "row", 16, [1, 2])
    total = xor_sum(total, "row", 16, [4, 8])
    total = xor_sum(total, "node", 8, [1, 2])
    total = xor_sum(total, "node", 8, [4])
    pick = lax.dynamic_slice_in_dim(assignment, node, 1)
    mine, gram = respond(pick, weights, total, hi, lo)

    full = jnp.zeros((16, PLANES, 128, LANES), F32)
    x = node % 4
    high_z = node // 4

    def put(full, piece, z, dx, first):
        where = (z * 4 + (x + dx + 4) % 4) * ROWS
        return lax.dynamic_update_slice(full, piece, (first, 0, where, 0))

    other = lax.ppermute(mine, "node", [(i, i ^ 4) for i in range(8)])
    for block, z in ((mine, high_z), (other, 1 - high_z)):
        left, right = turn(block, 1), turn(block, -1)
        far0, far1 = turn(left[:8], 1), turn(right[8:], -1)
        for piece, dx, first in ((block, 0, 0), (left, -1, 0), (right, 1, 0), (far0, 2, 0), (far1, 2, 8)):
            full = put(full, piece, z, dx, first)
    return full, gram[None, :, :16]


def solution(mesh):
    placed = (
        P(None, "row", None, None),
        P("row", None, None),
        P(None, "row", None, None),
        P(),
        P(),
        P(),
        P(),
    )
    return jax.shard_map(
        local,
        mesh=mesh,
        in_specs=placed,
        out_specs=(P(None, "row", None, None), P("node", None, None)),
        check_vma=False,
    )
```

```python
import jax
import jax.numpy as jnp
from jax import lax
from jax.experimental import pallas as pl
from jax.experimental.pallas import tpu as pltpu
from jax.sharding import PartitionSpec as P

QUAD = 8
COLS = 16
DEPTH = 5
PLANES = 4
ROWS = 16
WIDE = ROWS + 2 * DEPTH
SPAN = PLANES + 2 * DEPTH
LANES = 128
CELLS = 1048576.0
SEND_B = sum(WIDE - 2 * d for d in range(1, PLANES + 1)) * COLS
SEND_E = PLANES * 24
FAR_B = ROWS * COLS
OWN_B = PLANES * WIDE * COLS
F32 = jnp.float32
BF16 = jnp.bfloat16
VMEM = pl.BlockSpec(memory_space=pltpu.VMEM)
SMEM = pl.BlockSpec(memory_space=pltpu.SMEM)
ANY = pl.BlockSpec(memory_space=pl.ANY)


def pack_kernel(at_ref, src_ref, diag_ref, own_ref, fwd_ref, bwd_ref, fwd2_ref, bwd2_ref, edge_ref):
    edge_ref[...] = jnp.zeros_like(edge_ref)
    for x in range(PLANES):
        edge_ref[x, pl.ds(16, 128), :] = diag_ref[x] + 6.0

    def rows(dst_ref, base, plane, first, count):
        for q in range(count):
            y = jnp.clip(first + q, 0, 127)
            dst_ref[pl.ds(base + q * COLS, COLS), :] = src_ref[
                pl.ds(plane * 128 + y, COLS, stride=PLANES * 128), :
            ]

    own = at_ref[0]
    for x in range(PLANES):
        rows(own_ref, x * WIDE * COLS, x, own - DEPTH, WIDE)
        own_ref[pl.ds(OWN_B + x * 32, 32), :] = edge_ref[x, pl.ds(16 + own - DEPTH, 32), :]
    base = 0
    for d in range(1, PLANES + 1):
        count = WIDE - 2 * d
        for dst_ref, at, plane in ((fwd_ref, at_ref[1], PLANES - d), (bwd_ref, at_ref[2], d - 1)):
            rows(dst_ref, base, plane, at - DEPTH + d, count)
            dst_ref[pl.ds(SEND_B + (d - 1) * 24, 24), :] = edge_ref[
                plane, pl.ds(16 + at - DEPTH + d, 24), :
            ]
        base += count * COLS
    for dst_ref, at, plane in ((fwd2_ref, at_ref[3], PLANES - 1), (bwd2_ref, at_ref[4], 0)):
        rows(dst_ref, 0, plane, at, ROWS)
        dst_ref[pl.ds(FAR_B, ROWS), :] = edge_ref[plane, pl.ds(16 + at, ROWS), :]


def pack(at, inputs, diagonal):
    out = lambda n: jax.ShapeDtypeStruct((n, LANES), F32)
    return pl.pallas_call(
        pack_kernel,
        out_shape=(
            out(OWN_B + PLANES * 32),
            out(SEND_B + SEND_E),
            out(SEND_B + SEND_E),
            out(FAR_B + ROWS),
            out(FAR_B + ROWS),
        ),
        in_specs=[SMEM, VMEM, VMEM],
        out_specs=(VMEM,) * 5,
        scratch_shapes=[pltpu.VMEM((PLANES, 160, LANES), F32)],
        compiler_params=pltpu.CompilerParams(vmem_limit_bytes=24 << 20),
        name="pack",
    )(at, inputs.reshape(COLS * PLANES * 128, LANES), diagonal)


def solve_kernel(
    at_ref, freq_ref, count_ref, own_ref, low_ref, high_ref, low2_ref, high2_ref, obs_ref,
    hi_ref, lo_ref, part_ref,
    src, even, odd, near, edge, gre, gim, cat, obs, stage, sems,
):
    node = pl.program_id(0)

    @pl.when(node == 0)
    def _():
        copies = []

        def fetch(a, b):
            copies.append(pltpu.make_async_copy(a, b, sems.at[len(copies)]))
            copies[-1].start()

        fetch(obs_ref.at[:, :, pl.ds(pl.multiple_of(at_ref[0], 16), ROWS), :], obs)
        for x in range(PLANES):
            fetch(
                own_ref.at[pl.ds(x * WIDE * COLS, WIDE * COLS)],
                src.at[DEPTH + x],
            )
        fetch(own_ref.at[pl.ds(OWN_B, PLANES * 32)], stage.at[pl.ds(0, 128)])
        for s, (close, far) in enumerate(((low_ref, low2_ref), (high_ref, high2_ref))):
            base = 0
            for d in range(1, PLANES + 1):
                count = (WIDE - 2 * d) * COLS
                px = DEPTH - d if s == 0 else DEPTH + PLANES - 1 + d
                fetch(close.at[pl.ds(base, count)], src.at[px, pl.ds(d * COLS, count)])
                base += count
            px = 0 if s == 0 else SPAN - 1
            fetch(far.at[pl.ds(0, FAR_B)], src.at[px, pl.ds(DEPTH * COLS, FAR_B)])
            fetch(close.at[pl.ds(SEND_B, SEND_E)], stage.at[pl.ds(128 + s * 112, SEND_E)])
            fetch(far.at[pl.ds(FAR_B, ROWS)], stage.at[pl.ds(128 + s * 112 + 96, ROWS)])
        edge[...] = jnp.zeros_like(edge)
        part_ref[...] = jnp.zeros_like(part_ref)
        apart = lax.broadcasted_iota(jnp.int32, (LANES, LANES), 0) - lax.broadcasted_iota(
            jnp.int32, (LANES, LANES), 1
        )
        ones = jnp.where(jnp.abs(apart) == 1, 1.0, 0.0).astype(BF16)
        near[0:LANES, :] = ones
        near[LANES : 2 * LANES, :] = ones
        for c in copies:
            c.wait()
        for x in range(PLANES):
            edge[DEPTH + x] = stage[pl.ds(x * 32, 32), :]
            for y in range(ROWS):
                v = obs[:, x, y, :]
                hi = v.astype(BF16)
                at = pl.ds((x * ROWS + y) * LANES, LANES)
                cat[64:80, at] = hi
                cat[80:96, at] = (v - hi.astype(F32)).astype(BF16)
        for s in range(2):
            for d in range(1, DEPTH + 1):
                px = DEPTH - d if s == 0 else DEPTH + PLANES - 1 + d
                edge[px, pl.ds(d, WIDE - 2 * d), :] = stage[
                    pl.ds(128 + s * 112 + (d - 1) * 24, WIDE - 2 * d), :
                ]

    count = count_ref[node]
    freq = freq_ref[node]

    @pl.loop(0, SPAN)
    def _(px):
        d = edge[px]
        inv = 1.0 / (d * d + freq * freq)
        gre[px] = d * inv
        gim[px] = jnp.where(d > 0.0, -freq * inv, 0.0)

    def planes(level, top, m, body):
        dd = level - m
        idle = (dd < 0) | (level > top)
        trips = jnp.where(idle, 0, jnp.where(dd == 0, PLANES // 2, 1))

        @pl.loop(0, trips)
        def _(q):
            left = jnp.where(dd == 0, DEPTH + 2 * q, DEPTH - dd)
            right = jnp.where(dd == 0, left + 1, DEPTH + PLANES - 1 + dd)
            body(left, right)

    def spread(ref, px, r):
        return jnp.broadcast_to(ref[px, pl.ds(r, 1), :], (COLS, LANES))

    def at_row(r):
        return pl.ds(r * COLS, COLS)

    def halves(v):
        hi = v.astype(BF16)
        return hi, (v - hi.astype(F32)).astype(BF16)

    def begin(field):
        for m in range(DEPTH + 1):

            def first(*pair_of, m=m):
                for px in pair_of:
                    for r in range(DEPTH - m, DEPTH + ROWS + m):
                        b = src[px, at_row(r), :]
                        field[0, px, at_row(r), :] = spread(gre, px, r) * b
                        field[1, px, at_row(r), :] = spread(gim, px, r) * b

            planes(count - 1, count - 1, m, first)

    def sweep(old, new, level, depth):
        for m in range(depth):

            def body(*pair_of, m=m):
                start, rows = DEPTH - m, ROWS + 2 * m
                beside = []
                for px in pair_of:
                    lhs = []
                    for i in range(rows):
                        for c in range(2):
                            hi, lo = halves(old[c, px, at_row(start + i), :])
                            lhs.append(jnp.concatenate([hi, lo], 1))
                    beside.append(
                        jnp.dot(jnp.concatenate(lhs, 0), near[...], preferred_element_type=F32)
                    )
                for px, side in zip(pair_of, beside):

                    def get(c, p, r):
                        return old[c, p, at_row(r), :]

                    below = [get(c, px, start - 1) for c in range(2)]
                    here = [get(c, px, start) for c in range(2)]
                    for i in range(rows):
                        r = start + i
                        above = [get(c, px, r + 1) for c in range(2)]
                        re, im = [
                            (get(c, px - 1, r) + get(c, px + 1, r))
                            + (below[c] + above[c])
                            + side[i * 32 + c * COLS : i * 32 + c * COLS + COLS]
                            for c in range(2)
                        ]
                        re = re + src[px, at_row(r), :]
                        p, q = spread(gre, px, r), spread(gim, px, r)
                        new[0, px, at_row(r), :] = p * re - q * im
                        new[1, px, at_row(r), :] = p * im + q * re
                        below, here = here, above

            planes(level, count - 2, m, body)

    @pl.when(lax.rem(count, 2) == 1)
    def _():
        begin(even)

    @pl.when(lax.rem(count, 2) == 0)
    def _():
        begin(odd)

    @pl.loop(0, 3)
    def _(t):
        sweep(odd, even, 4 - 2 * t, DEPTH)
        sweep(even, odd, 3 - 2 * t, DEPTH - 1)

    @pl.loop(0, PLANES)
    def _(x):
        for y in range(ROWS):
            at = pl.ds(pl.multiple_of(x * (ROWS * LANES) + y * LANES, LANES), LANES)
            for c in range(2):
                hi, lo = halves(even[c, DEPTH + x, at_row(DEPTH + y), :])
                cat[pl.ds(c * COLS, COLS), at] = hi
                cat[pl.ds(32 + c * COLS, COLS), at] = lo
                hi_ref[pl.ds(c * COLS, COLS), at] = hi
                lo_ref[pl.ds(c * COLS, COLS), at] = lo

    o = lax.dot_general(
        cat[...], cat[0:64, :], (((1,), (1,)), ((), ())), preferred_element_type=F32
    )
    o = jnp.concatenate([o, jnp.zeros((96, 64), F32)], 1)
    lane = lax.broadcasted_iota(jnp.int32, (COLS, LANES), 1)
    proj = o[64:80] + pltpu.roll(o[64:80], LANES - 32, 1) + o[80:96]
    proj = pltpu.roll(jnp.where(lane < 32, proj, 0.0), 32 * lax.rem(node, 4), 1)
    part_ref[pl.ds(pl.multiple_of(16 * (node // 4), 16), 16), :] += proj
    gu = o[0:16] + pltpu.roll(o[0:16], LANES - 32, 1) + o[32:48]
    gw = o[16:32] + pltpu.roll(o[16:32], LANES - 32, 1) + o[48:64]
    gram = jnp.where(lane < 16, gu + pltpu.roll(gw, LANES - 16, 1), 0.0)
    part_ref[32:48, :] += pltpu.roll(gram, 16 * node, 1)


def solve(at, freqs, counts, own, low, high, low2, high2, obs):
    cells = PLANES * ROWS * LANES
    return pl.pallas_call(
        solve_kernel,
        grid=(QUAD,),
        out_shape=(
            jax.ShapeDtypeStruct((QUAD * 32, cells), BF16),
            jax.ShapeDtypeStruct((QUAD * 32, cells), BF16),
            jax.ShapeDtypeStruct((48, LANES), F32),
        ),
        in_specs=[SMEM, SMEM, SMEM] + [ANY] * 6,
        out_specs=(
            pl.BlockSpec((32, cells), lambda k: (k, 0)),
            pl.BlockSpec((32, cells), lambda k: (k, 0)),
            pl.BlockSpec((48, LANES), lambda k: (0, 0)),
        ),
        scratch_shapes=[
            pltpu.VMEM((SPAN, WIDE * COLS, LANES), F32),
            pltpu.VMEM((2, SPAN, WIDE * COLS, LANES), F32),
            pltpu.VMEM((2, SPAN, WIDE * COLS, LANES), F32),
            pltpu.VMEM((2 * LANES, LANES), BF16),
            pltpu.VMEM((SPAN, 32, LANES), F32),
            pltpu.VMEM((SPAN, 32, LANES), F32),
            pltpu.VMEM((SPAN, 32, LANES), F32),
            pltpu.VMEM((96, cells), BF16),
            pltpu.VMEM((COLS, PLANES, ROWS, LANES), F32),
            pltpu.VMEM((352, LANES), F32),
            pltpu.SemaphoreType.DMA((24,)),
        ],
        compiler_params=pltpu.CompilerParams(
            dimension_semantics=("arbitrary",), vmem_limit_bytes=60 << 20
        ),
        name="solve",
    )(at, freqs, counts, own, low, high, low2, high2, obs)


def respond_kernel(pick_ref, weight_ref, sum_ref, hi_ref, lo_ref, out_ref, gram_ref, coef):
    @pl.when(pl.program_id(0) == 0)
    def _():
        lane = lax.broadcasted_iota(jnp.int32, (16, LANES), 1)
        for half in range(2):
            scale = weight_ref[half * 4] * (1.0 / QUAD)
            for j in range(1, 4):
                scale = jnp.where(lane < 32 * j, scale, weight_ref[half * 4 + j] * (1.0 / QUAD))
            acc = sum_ref[16 * half : 16 * half + 16, :] * scale
            at = pl.ds(half * LANES, LANES)
            hi = acc.astype(BF16)
            coef[0:16, at] = hi
            coef[16:32, at] = (acc - hi.astype(F32)).astype(BF16)
        node = pick_ref[0]
        gram = pltpu.roll(sum_ref[32:48, :], lax.rem(128 - 16 * node, 128), 1)
        gram_ref[...] = gram * (weight_ref[node] * (1.0 / CELLS))

    big = jnp.dot(coef[...], hi_ref[...], preferred_element_type=F32)
    small = jnp.dot(coef[0:16, :], lo_ref[...], preferred_element_type=F32)
    res = big[0:16] + big[16:32] + small
    for y in range(ROWS):
        out_ref[:, 0, y, :] = res[:, y * LANES : (y + 1) * LANES]


def respond(pick, weights, total, hi, lo):
    wide = ROWS * LANES
    return pl.pallas_call(
        respond_kernel,
        grid=(PLANES,),
        out_shape=(
            jax.ShapeDtypeStruct((16, PLANES, ROWS, LANES), F32),
            jax.ShapeDtypeStruct((16, LANES), F32),
        ),
        in_specs=[
            SMEM,
            SMEM,
            pl.BlockSpec((48, LANES), lambda x: (0, 0)),
            pl.BlockSpec((QUAD * 32, wide), lambda x: (0, x)),
            pl.BlockSpec((QUAD * 32, wide), lambda x: (0, x)),
        ],
        out_specs=(
            pl.BlockSpec((16, 1, ROWS, LANES), lambda x: (0, x, 0, 0)),
            pl.BlockSpec((16, LANES), lambda x: (0, 0)),
        ),
        scratch_shapes=[pltpu.VMEM((32, QUAD * 32), BF16)],
        compiler_params=pltpu.CompilerParams(
            dimension_semantics=("arbitrary",), vmem_limit_bytes=60 << 20
        ),
        name="respond",
    )(pick, weights, total, hi, lo)


def step_pairs(step):
    pairs = []
    for node in range(8):
        for r in range(16):
            t = r + step
            if 0 <= t < 16:
                c, ct = r // 2, t // 2
                flip = c != ct and (c % 2 == 1 if step > 0 else c % 2 == 0)
                pairs.append((node * 16 + r, (node ^ 4 if flip else node) * 16 + t))
    return pairs


def xor_sum(x, axis, size, masks):
    combos = [0]
    for m in masks:
        combos += [c ^ m for c in combos]
    got = [x if c == 0 else lax.ppermute(x, axis, [(i, i ^ c) for i in range(size)]) for c in combos]
    while len(got) > 1:
        got = [got[i] + got[i + 1] for i in range(0, len(got), 2)]
    return got[0]


def turn(v, by):
    return lax.ppermute(v, "node", [(i, i // 4 * 4 + (i + by) % 4) for i in range(8)])


def local(inputs, diagonal, observations, frequencies, weights, counts, assignment):
    node = lax.axis_index("node")
    row = lax.axis_index("row")
    core, odd = row % 2, (row // 2) % 2
    fwd2 = node ^ (4 * odd)
    bwd2 = node ^ (4 * (1 - odd))
    fwd = jnp.where(core == 1, fwd2, node)
    bwd = jnp.where(core == 0, bwd2, node)
    at = (16 * jnp.stack([node, fwd, bwd, fwd2, bwd2])).astype(jnp.int32)
    own, s1, s2, s3, s4 = pack(at, inputs, diagonal)
    both = ("node", "row")
    low = lax.ppermute(s1, both, step_pairs(1))
    high = lax.ppermute(s2, both, step_pairs(-1))
    low2 = lax.ppermute(s3, both, step_pairs(2))
    high2 = lax.ppermute(s4, both, step_pairs(-2))
    hi, lo, part = solve(at, frequencies, counts, own, low, high, low2, high2, observations)
    total = xor_sum(part, "row", 16, [1, 2])
    total = xor_sum(total, "row", 16, [4, 8])
    total = xor_sum(total, "node", 8, [1, 2])
    total = xor_sum(total, "node", 8, [4])
    pick = lax.dynamic_slice_in_dim(assignment, node, 1)
    mine, gram = respond(pick, weights, total, hi, lo)

    full = jnp.zeros((16, PLANES, 128, LANES), F32)
    x = node % 4
    high_z = node // 4

    def put(full, piece, z, dx, first):
        where = (z * 4 + (x + dx + 4) % 4) * ROWS
        return lax.dynamic_update_slice(full, piece, (first, 0, where, 0))

    other = lax.ppermute(mine, "node", [(i, i ^ 4) for i in range(8)])
    for block, z in ((mine, high_z), (other, 1 - high_z)):
        left, right = turn(block, 1), turn(block, -1)
        far0, far1 = turn(left[:8], 1), turn(right[8:], -1)
        for piece, dx, first in ((block, 0, 0), (left, -1, 0), (right, 1, 0), (far0, 2, 0), (far1, 2, 8)):
            full = put(full, piece, z, dx, first)
    return full, gram[None, :, :16]


def solution(mesh):
    placed = (
        P(None, "row", None, None),
        P("row", None, None),
        P(None, "row", None, None),
        P(),
        P(),
        P(),
        P(),
    )
    return jax.shard_map(
        local,
        mesh=mesh,
        in_specs=placed,
        out_specs=(P(None, "row", None, None), P("node", None, None)),
        check_vma=False,
    )
```

```python
import jax
import jax.numpy as jnp
from jax import lax
from jax.experimental import pallas as pl
from jax.experimental.pallas import tpu as pltpu
from jax.sharding import PartitionSpec as P

QUAD = 8
COLS = 16
DEPTH = 5
PLANES = 4
ROWS = 16
WIDE = ROWS + 2 * DEPTH
SPAN = PLANES + 2 * DEPTH
LANES = 128
CELLS = 1048576.0
SEND_B = sum(WIDE - 2 * d for d in range(1, PLANES + 1)) * COLS
SEND_E = PLANES * 24
FAR_B = ROWS * COLS
OWN_B = PLANES * WIDE * COLS
PACK_LIMIT = 58 << 20
SOLVE_LIMIT = 55 << 20
F32 = jnp.float32
BF16 = jnp.bfloat16
VMEM = pl.BlockSpec(memory_space=pltpu.VMEM)
SMEM = pl.BlockSpec(memory_space=pltpu.SMEM)
ANY = pl.BlockSpec(memory_space=pl.ANY)


def window(ref, start):
    return ref.at[:, :, pl.ds(pl.multiple_of(start, 8), 32), :]


def first_row(at):
    return jnp.clip(at - 8, 0, 96)


def fill_edge(edge_ref, diag_ref):
    for x in range(PLANES):
        edge_ref[x, pl.ds(0, 16), :] = jnp.zeros((16, LANES), F32)
        edge_ref[x, pl.ds(144, 16), :] = jnp.zeros((16, LANES), F32)
        edge_ref[x, pl.ds(16, 128), :] = diag_ref[x] + 6.0


def turned_rows(dst_ref, base, flat_ref, offset, first, count):
    for q in range(count):
        y = jnp.clip(first + q, 0, 127) + offset
        dst_ref[pl.ds(base + q * COLS, COLS), :] = flat_ref[
            pl.ds(y, COLS, stride=PLANES * 32), :
        ]


def pack_kernel(
    at_ref, src_ref, diag_ref, fwd_ref, bwd_ref, fwd2_ref, bwd2_ref, edge_ref, win, sems
):
    mine = at_ref[0]
    other = jnp.where(mine >= 64, mine - 64, mine + 64)
    copies = [
        pltpu.make_async_copy(window(src_ref, first_row(t)), win.at[w], sems.at[w])
        for w, t in enumerate((mine, other))
    ]
    for c in copies:
        c.start()
    fill_edge(edge_ref, diag_ref)
    for c in copies:
        c.wait()
    flat = win.reshape(2 * COLS * PLANES * 32, LANES)

    def send(dst_ref, base, at, plane, d, count):
        offset = jnp.where(at == mine, 0, COLS * PLANES * 32) + plane * 32 - first_row(at)
        turned_rows(dst_ref, base, flat, offset, at - DEPTH + d, count)

    base = 0
    for d in range(1, PLANES + 1):
        count = WIDE - 2 * d
        for dst_ref, at, plane in ((fwd_ref, at_ref[1], PLANES - d), (bwd_ref, at_ref[2], d - 1)):
            send(dst_ref, base, at, plane, d, count)
            dst_ref[pl.ds(SEND_B + (d - 1) * 24, 24), :] = edge_ref[
                plane, pl.ds(16 + at - DEPTH + d, 24), :
            ]
        base += count * COLS
    for dst_ref, at, plane in ((fwd2_ref, at_ref[3], PLANES - 1), (bwd2_ref, at_ref[4], 0)):
        send(dst_ref, 0, at, plane, DEPTH, ROWS)
        dst_ref[pl.ds(FAR_B, ROWS), :] = edge_ref[plane, pl.ds(16 + at, ROWS), :]


def pack(at, inputs, diagonal):
    out = lambda n: jax.ShapeDtypeStruct((n, LANES), F32)
    return pl.pallas_call(
        pack_kernel,
        out_shape=(
            out(SEND_B + SEND_E),
            out(SEND_B + SEND_E),
            out(FAR_B + ROWS),
            out(FAR_B + ROWS),
        ),
        in_specs=[SMEM, ANY, VMEM],
        out_specs=(VMEM,) * 4,
        scratch_shapes=[
            pltpu.VMEM((PLANES, 160, LANES), F32),
            pltpu.VMEM((2, COLS, PLANES, 32, LANES), F32),
            pltpu.SemaphoreType.DMA((2,)),
        ],
        compiler_params=pltpu.CompilerParams(vmem_limit_bytes=PACK_LIMIT),
        name="pack",
    )(at, inputs, diagonal)


def prep_kernel(at_ref, src_ref, diag_ref, obs_ref, after_ref, own_ref, probe_ref, edge_ref, win, obs, sems):
    mine = at_ref[0]
    copies = (
        pltpu.make_async_copy(window(src_ref, first_row(mine)), win, sems.at[0]),
        pltpu.make_async_copy(
            obs_ref.at[:, :, pl.ds(pl.multiple_of(mine, 16), ROWS), :], obs, sems.at[1]
        ),
    )
    for c in copies:
        c.start()
    fill_edge(edge_ref, diag_ref)
    for c in copies:
        c.wait()
    flat = win.reshape(COLS * PLANES * 32, LANES)
    seen = obs.reshape(COLS * PLANES * ROWS, LANES)
    for x in range(PLANES):
        offset = x * 32 - first_row(mine)
        turned_rows(own_ref, x * WIDE * COLS, flat, offset, mine - DEPTH, WIDE)
        own_ref[pl.ds(OWN_B + x * 32, 32), :] = edge_ref[x, pl.ds(16 + mine - DEPTH, 32), :]
        for y in range(ROWS):
            v = seen[pl.ds(x * ROWS + y, COLS, stride=PLANES * ROWS), :]
            hi = v.astype(BF16)
            at = pl.ds((x * ROWS + y) * LANES, LANES)
            probe_ref[0:16, at] = hi
            probe_ref[16:32, at] = (v - hi.astype(F32)).astype(BF16)


def prep(at, inputs, diagonal, observations, after):
    return pl.pallas_call(
        prep_kernel,
        out_shape=(
            jax.ShapeDtypeStruct((OWN_B + PLANES * 32, LANES), F32),
            jax.ShapeDtypeStruct((32, PLANES * ROWS * LANES), BF16),
        ),
        in_specs=[SMEM, ANY, VMEM, ANY, ANY],
        out_specs=(VMEM, VMEM),
        scratch_shapes=[
            pltpu.VMEM((PLANES, 160, LANES), F32),
            pltpu.VMEM((COLS, PLANES, 32, LANES), F32),
            pltpu.VMEM((COLS, PLANES, ROWS, LANES), F32),
            pltpu.SemaphoreType.DMA((2,)),
        ],
        compiler_params=pltpu.CompilerParams(vmem_limit_bytes=PACK_LIMIT),
        cost_estimate=pl.CostEstimate(flops=40_000_000, bytes_accessed=4_000_000, transcendentals=0),
        name="prep",
    )(at, inputs, diagonal, observations, after)


def solve_kernel(
    freq_ref, count_ref, own_ref, low_ref, high_ref, low2_ref, high2_ref, probe_ref,
    full_ref, part_ref,
    src, even, odd, near, edge, gre, gim, cat, stage, sems, out_sem,
):
    node = pl.program_id(0)

    @pl.when(node == 0)
    def _():
        copies = []

        def fetch(a, b):
            copies.append(pltpu.make_async_copy(a, b, sems.at[len(copies)]))
            copies[-1].start()

        fetch(probe_ref, cat.at[pl.ds(64, 32)])
        for x in range(PLANES):
            fetch(
                own_ref.at[pl.ds(x * WIDE * COLS, WIDE * COLS)],
                src.at[DEPTH + x],
            )
        fetch(own_ref.at[pl.ds(OWN_B, PLANES * 32)], stage.at[pl.ds(0, 128)])
        for s, (close, far) in enumerate(((low_ref, low2_ref), (high_ref, high2_ref))):
            base = 0
            for d in range(1, PLANES + 1):
                count = (WIDE - 2 * d) * COLS
                px = DEPTH - d if s == 0 else DEPTH + PLANES - 1 + d
                fetch(close.at[pl.ds(base, count)], src.at[px, pl.ds(d * COLS, count)])
                base += count
            px = 0 if s == 0 else SPAN - 1
            fetch(far.at[pl.ds(0, FAR_B)], src.at[px, pl.ds(DEPTH * COLS, FAR_B)])
            fetch(close.at[pl.ds(SEND_B, SEND_E)], stage.at[pl.ds(128 + s * 112, SEND_E)])
            fetch(far.at[pl.ds(FAR_B, ROWS)], stage.at[pl.ds(128 + s * 112 + 96, ROWS)])
        edge[...] = jnp.zeros_like(edge)
        part_ref[...] = jnp.zeros_like(part_ref)
        apart = lax.broadcasted_iota(jnp.int32, (LANES, LANES), 0) - lax.broadcasted_iota(
            jnp.int32, (LANES, LANES), 1
        )
        ones = jnp.where(jnp.abs(apart) == 1, 1.0, 0.0).astype(BF16)
        near[0:LANES, :] = ones
        near[LANES : 2 * LANES, :] = ones
        for c in copies:
            c.wait()
        for x in range(PLANES):
            edge[DEPTH + x] = stage[pl.ds(x * 32, 32), :]
        for s in range(2):
            for d in range(1, DEPTH + 1):
                px = DEPTH - d if s == 0 else DEPTH + PLANES - 1 + d
                edge[px, pl.ds(d, WIDE - 2 * d), :] = stage[
                    pl.ds(128 + s * 112 + (d - 1) * 24, WIDE - 2 * d), :
                ]

    count = count_ref[node]
    freq = freq_ref[node]

    for px in range(SPAN):
        d = edge[px]
        inv = 1.0 / (d * d + freq * freq)
        gre[px] = d * inv
        gim[px] = jnp.where(d > 0.0, -freq * inv, 0.0)

    def planes(level, top, m, body):
        dd = level - m
        idle = (dd < 0) | (level > top)
        trips = jnp.where(idle, 0, jnp.where(dd == 0, PLANES // 2, 1))

        @pl.loop(0, trips)
        def _(q):
            left = jnp.where(dd == 0, DEPTH + 2 * q, DEPTH - dd)
            right = jnp.where(dd == 0, left + 1, DEPTH + PLANES - 1 + dd)
            body(left, right)

    def spread(ref, px, r):
        return jnp.broadcast_to(ref[px, pl.ds(r, 1), :], (COLS, LANES))

    def at_row(r):
        return pl.ds(r * COLS, COLS)

    def halves(v):
        hi = v.astype(BF16)
        return hi, (v - hi.astype(F32)).astype(BF16)

    def begin(field):
        for m in range(DEPTH + 1):

            def first(*pair_of, m=m):
                for px in pair_of:
                    for r in range(DEPTH - m, DEPTH + ROWS + m):
                        b = src[px, at_row(r), :]
                        field[0, px, at_row(r), :] = spread(gre, px, r) * b
                        field[1, px, at_row(r), :] = spread(gim, px, r) * b

            planes(count - 1, count - 1, m, first)

    def sweep(old, new, level, depth):
        for m in range(depth):

            def body(*pair_of, m=m):
                start, rows = DEPTH - m, ROWS + 2 * m
                beside = []
                for px in pair_of:
                    lhs = []
                    for i in range(rows):
                        for c in range(2):
                            hi, lo = halves(old[c, px, at_row(start + i), :])
                            lhs.append(jnp.concatenate([hi, lo], 1))
                    beside.append(
                        jnp.dot(jnp.concatenate(lhs, 0), near[...], preferred_element_type=F32)
                    )
                for px, side in zip(pair_of, beside):

                    def get(c, p, r):
                        return old[c, p, at_row(r), :]

                    below = [get(c, px, start - 1) for c in range(2)]
                    here = [get(c, px, start) for c in range(2)]
                    for i in range(rows):
                        r = start + i
                        above = [get(c, px, r + 1) for c in range(2)]
                        re, im = [
                            (get(c, px - 1, r) + get(c, px + 1, r))
                            + (below[c] + above[c])
                            + side[i * 32 + c * COLS : i * 32 + c * COLS + COLS]
                            for c in range(2)
                        ]
                        re = re + src[px, at_row(r), :]
                        p, q = spread(gre, px, r), spread(gim, px, r)
                        new[0, px, at_row(r), :] = p * re - q * im
                        new[1, px, at_row(r), :] = p * im + q * re
                        below, here = here, above

            planes(level, count - 2, m, body)

    @pl.when(lax.rem(count, 2) == 1)
    def _():
        begin(even)

    @pl.when(lax.rem(count, 2) == 0)
    def _():
        begin(odd)

    @pl.loop(0, 3)
    def _(t):
        sweep(odd, even, 4 - 2 * t, DEPTH)
        sweep(even, odd, 3 - 2 * t, DEPTH - 1)

    leave = pltpu.make_async_copy(
        cat.at[pl.ds(0, 64)],
        full_ref.at[pl.ds(pl.multiple_of(64 * node, 64), 64)],
        out_sem,
    )

    @pl.when(node > 0)
    def _():
        leave.wait()

    @pl.loop(0, PLANES)
    def _(x):
        for y in range(ROWS):
            at = pl.ds(pl.multiple_of(x * (ROWS * LANES) + y * LANES, LANES), LANES)
            for c in range(2):
                hi, lo = halves(even[c, DEPTH + x, at_row(DEPTH + y), :])
                cat[pl.ds(c * COLS, COLS), at] = hi
                cat[pl.ds(32 + c * COLS, COLS), at] = lo

    leave.start()
    o = lax.dot_general(
        cat[...], cat[0:64, :], (((1,), (1,)), ((), ())), preferred_element_type=F32
    )
    o = jnp.concatenate([o, jnp.zeros((96, 64), F32)], 1)
    lane = lax.broadcasted_iota(jnp.int32, (COLS, LANES), 1)
    proj = o[64:80] + pltpu.roll(o[64:80], LANES - 32, 1) + o[80:96]
    proj = pltpu.roll(jnp.where(lane < 32, proj, 0.0), 32 * lax.rem(node, 4), 1)
    part_ref[pl.ds(pl.multiple_of(16 * (node // 4), 16), 16), :] += proj
    gu = o[0:16] + pltpu.roll(o[0:16], LANES - 32, 1) + o[32:48]
    gw = o[16:32] + pltpu.roll(o[16:32], LANES - 32, 1) + o[48:64]
    gram = jnp.where(lane < 16, gu + pltpu.roll(gw, LANES - 16, 1), 0.0)
    part_ref[32:48, :] += pltpu.roll(gram, 16 * node, 1)

    @pl.when(node == QUAD - 1)
    def _():
        leave.wait()


def solve(freqs, counts, own, low, high, low2, high2, probe):
    cells = PLANES * ROWS * LANES
    return pl.pallas_call(
        solve_kernel,
        grid=(QUAD,),
        out_shape=(
            jax.ShapeDtypeStruct((QUAD * 64, cells), BF16),
            jax.ShapeDtypeStruct((48, LANES), F32),
        ),
        in_specs=[SMEM, SMEM] + [ANY] * 6,
        out_specs=(
            pl.BlockSpec(memory_space=pltpu.HBM),
            pl.BlockSpec((48, LANES), lambda k: (0, 0)),
        ),
        scratch_shapes=[
            pltpu.VMEM((SPAN, WIDE * COLS, LANES), F32),
            pltpu.VMEM((2, SPAN, WIDE * COLS, LANES), F32),
            pltpu.VMEM((2, SPAN, WIDE * COLS, LANES), F32),
            pltpu.VMEM((2 * LANES, LANES), BF16),
            pltpu.VMEM((SPAN, 32, LANES), F32),
            pltpu.VMEM((SPAN, 32, LANES), F32),
            pltpu.VMEM((SPAN, 32, LANES), F32),
            pltpu.VMEM((96, cells), BF16),
            pltpu.VMEM((352, LANES), F32),
            pltpu.SemaphoreType.DMA((24,)),
            pltpu.SemaphoreType.DMA,
        ],
        compiler_params=pltpu.CompilerParams(
            dimension_semantics=("arbitrary",), vmem_limit_bytes=SOLVE_LIMIT
        ),
        name="solve",
    )(freqs, counts, own, low, high, low2, high2, probe)


def respond_kernel(pick_ref, weight_ref, sum_ref, full_ref, out_ref, gram_ref, coef):
    @pl.when(pl.program_id(0) == 0)
    def _():
        lane = lax.broadcasted_iota(jnp.int32, (16, LANES), 1)
        for half in range(2):
            scale = weight_ref[half * 4] * (1.0 / QUAD)
            for j in range(1, 4):
                scale = jnp.where(lane < 32 * j, scale, weight_ref[half * 4 + j] * (1.0 / QUAD))
            acc = sum_ref[16 * half : 16 * half + 16, :] * scale
            for b in range(2):
                one = pltpu.roll(acc, 64, 1) if b else acc
                twice = jnp.where(
                    lane < 32,
                    one,
                    jnp.where(lane < 96, pltpu.roll(one, 32, 1), pltpu.roll(one, 64, 1)),
                )
                at = pl.ds((half * 2 + b) * LANES, LANES)
                hi = twice.astype(BF16)
                coef[0:16, at] = hi
                coef[16:32, at] = (twice - hi.astype(F32)).astype(BF16)
        node = pick_ref[0]
        gram = pltpu.roll(sum_ref[32:48, :], lax.rem(128 - 16 * node, 128), 1)
        gram_ref[...] = gram * (weight_ref[node] * (1.0 / CELLS))

    big = jnp.dot(coef[...], full_ref[...], preferred_element_type=F32)
    res = big[0:16] + big[16:32]
    for y in range(ROWS):
        out_ref[:, 0, y, :] = res[:, y * LANES : (y + 1) * LANES]


def respond(pick, weights, total, full):
    wide = ROWS * LANES
    return pl.pallas_call(
        respond_kernel,
        grid=(PLANES,),
        out_shape=(
            jax.ShapeDtypeStruct((16, PLANES, ROWS, LANES), F32),
            jax.ShapeDtypeStruct((16, LANES), F32),
        ),
        in_specs=[
            SMEM,
            SMEM,
            pl.BlockSpec((48, LANES), lambda x: (0, 0)),
            pl.BlockSpec((QUAD * 64, wide), lambda x: (0, x)),
        ],
        out_specs=(
            pl.BlockSpec((16, 1, ROWS, LANES), lambda x: (0, x, 0, 0)),
            pl.BlockSpec((16, LANES), lambda x: (0, 0)),
        ),
        scratch_shapes=[pltpu.VMEM((32, QUAD * 64), BF16)],
        compiler_params=pltpu.CompilerParams(
            dimension_semantics=("arbitrary",), vmem_limit_bytes=58 << 20
        ),
        name="respond",
    )(pick, weights, total, full)


def step_pairs(step):
    pairs = []
    for node in range(8):
        for r in range(16):
            t = r + step
            if 0 <= t < 16:
                c, ct = r // 2, t // 2
                flip = c != ct and (c % 2 == 1 if step > 0 else c % 2 == 0)
                pairs.append((node * 16 + r, (node ^ 4 if flip else node) * 16 + t))
    return pairs


def xor_sum(x, axis, size, masks):
    combos = [0]
    for m in masks:
        combos += [c ^ m for c in combos]
    got = [x if c == 0 else lax.ppermute(x, axis, [(i, i ^ c) for i in range(size)]) for c in combos]
    while len(got) > 1:
        got = [got[i] + got[i + 1] for i in range(0, len(got), 2)]
    return got[0]


def turn(v, by):
    return lax.ppermute(v, "node", [(i, i // 4 * 4 + (i + by) % 4) for i in range(8)])


def across(v):
    return lax.ppermute(v, "node", [(i, i ^ 4) for i in range(8)])


def place_kernel(spot_ref, *refs):
    pieces, out_ref, sems = refs[:10], refs[10], refs[11]
    copies = []
    for g in range(2):
        for k, (slot, first) in enumerate(((0, 0), (1, 0), (2, 0), (3, 0), (3, 8))):
            piece = pieces[g * 5 + k]
            at = pl.multiple_of(spot_ref[g * 4 + slot], ROWS)
            dst = out_ref.at[pl.ds(first, piece.shape[0]), :, pl.ds(at, ROWS), :]
            copies.append(pltpu.make_async_copy(piece, dst, sems.at[g * 5 + k]))
    for c in copies:
        c.start()
    for c in copies:
        c.wait()


def place(spots, pieces):
    return pl.pallas_call(
        place_kernel,
        out_shape=jax.ShapeDtypeStruct((16, PLANES, 128, LANES), F32),
        in_specs=[SMEM] + [ANY] * 10,
        out_specs=pl.BlockSpec(memory_space=pltpu.HBM),
        scratch_shapes=[pltpu.SemaphoreType.DMA((10,))],
        compiler_params=pltpu.CompilerParams(vmem_limit_bytes=1 << 20),
        name="place",
    )(spots, *pieces)


def local(inputs, diagonal, observations, frequencies, weights, counts, assignment):
    node = lax.axis_index("node")
    row = lax.axis_index("row")
    core, odd = row % 2, (row // 2) % 2
    fwd2 = node ^ (4 * odd)
    bwd2 = node ^ (4 * (1 - odd))
    fwd = jnp.where(core == 1, fwd2, node)
    bwd = jnp.where(core == 0, bwd2, node)
    at = (16 * jnp.stack([node, fwd, bwd, fwd2, bwd2])).astype(jnp.int32)
    s1, s2, s3, s4 = pack(at, inputs, diagonal)
    own, probe = prep(at, inputs, diagonal, observations, s3)
    both = ("node", "row")
    low = lax.ppermute(s1, both, step_pairs(1))
    high = lax.ppermute(s2, both, step_pairs(-1))
    low2 = lax.ppermute(s3, both, step_pairs(2))
    high2 = lax.ppermute(s4, both, step_pairs(-2))
    fields, part = solve(frequencies, counts, own, low, high, low2, high2, probe)
    total = xor_sum(part, "row", 16, [1, 2])
    total = xor_sum(total, "row", 16, [4, 8])
    total = xor_sum(total, "node", 8, [1, 2])
    total = xor_sum(total, "node", 8, [4])
    pick = lax.dynamic_slice_in_dim(assignment, node, 1)
    mine, gram = respond(pick, weights, total, fields)

    left, right, other = turn(mine, 1), turn(mine, -1), across(mine)
    far0, far1 = turn(left[:8], 1), turn(right[8:], -1)
    left_o, right_o = turn(other, 1), turn(other, -1)
    far0_o, far1_o = across(far0), across(far1)
    x, z = node % 4, node // 4
    spots = []
    for side in (z, 1 - z):
        spots += [(side * 4 + (x + dx) % 4) * ROWS for dx in (0, 3, 1, 2)]
    full = place(
        jnp.stack(spots).astype(jnp.int32),
        (mine, left, right, far0, far1, other, left_o, right_o, far0_o, far1_o),
    )
    return full, gram[None, :, :16]


def solution(mesh):
    placed = (
        P(None, "row", None, None),
        P("row", None, None),
        P(None, "row", None, None),
        P(),
        P(),
        P(),
        P(),
    )
    return jax.shard_map(
        local,
        mesh=mesh,
        in_specs=placed,
        out_specs=(P(None, "row", None, None), P("node", None, None)),
        check_vma=False,
    )
```

```python
import jax
import jax.numpy as jnp
from jax import lax
from jax.experimental import pallas as pl
from jax.experimental.pallas import tpu as pltpu
from jax.sharding import PartitionSpec as P

QUAD = 8
COLS = 16
DEPTH = 5
PLANES = 4
ROWS = 16
WIDE = ROWS + 2 * DEPTH
SPAN = PLANES + 2 * DEPTH
LANES = 128
CELLS = 1048576.0
SEND_B = sum(WIDE - 2 * d for d in range(1, PLANES + 1)) * COLS
SEND_E = PLANES * 24
FAR_B = ROWS * COLS
OWN_B = PLANES * WIDE * COLS
STEP = 16
PACK_LIMIT = 50 << 20
SOLVE_LIMIT = 51 << 20
F32 = jnp.float32
BF16 = jnp.bfloat16
VMEM = pl.BlockSpec(memory_space=pltpu.VMEM)
SMEM = pl.BlockSpec(memory_space=pltpu.SMEM)
ANY = pl.BlockSpec(memory_space=pl.ANY)


def window(ref, start):
    return ref.at[:, :, pl.ds(pl.multiple_of(start, 8), 32), :]


def first_row(at):
    return jnp.clip(at - 8, 0, 96)


def fill_edge(edge_ref, diag_ref):
    for x in range(PLANES):
        edge_ref[x, pl.ds(0, 16), :] = jnp.zeros((16, LANES), F32)
        edge_ref[x, pl.ds(144, 16), :] = jnp.zeros((16, LANES), F32)
        edge_ref[x, pl.ds(16, 128), :] = diag_ref[x] + 6.0


def turned_rows(dst_ref, base, flat_ref, offset, first, count):
    for q in range(count):
        y = jnp.clip(first + q, 0, 127) + offset
        dst_ref[pl.ds(base + q * COLS, COLS), :] = flat_ref[
            pl.ds(y, COLS, stride=PLANES * 32), :
        ]


def pack_kernel(
    at_ref, src_ref, diag_ref, fwd_ref, bwd_ref, fwd2_ref, bwd2_ref, edge_ref, win, sems
):
    mine = at_ref[0]
    other = jnp.where(mine >= 64, mine - 64, mine + 64)
    copies = [
        pltpu.make_async_copy(window(src_ref, first_row(t)), win.at[w], sems.at[w])
        for w, t in enumerate((mine, other))
    ]
    for c in copies:
        c.start()
    fill_edge(edge_ref, diag_ref)
    for c in copies:
        c.wait()
    flat = win.reshape(2 * COLS * PLANES * 32, LANES)

    def send(dst_ref, base, at, plane, d, count):
        offset = jnp.where(at == mine, 0, COLS * PLANES * 32) + plane * 32 - first_row(at)
        turned_rows(dst_ref, base, flat, offset, at - DEPTH + d, count)

    base = 0
    for d in range(1, PLANES + 1):
        count = WIDE - 2 * d
        for dst_ref, at, plane in ((fwd_ref, at_ref[1], PLANES - d), (bwd_ref, at_ref[2], d - 1)):
            send(dst_ref, base, at, plane, d, count)
            dst_ref[pl.ds(SEND_B + (d - 1) * 24, 24), :] = edge_ref[
                plane, pl.ds(16 + at - DEPTH + d, 24), :
            ]
        base += count * COLS
    for dst_ref, at, plane in ((fwd2_ref, at_ref[3], PLANES - 1), (bwd2_ref, at_ref[4], 0)):
        send(dst_ref, 0, at, plane, DEPTH, ROWS)
        dst_ref[pl.ds(FAR_B, ROWS), :] = edge_ref[plane, pl.ds(16 + at, ROWS), :]


def pack(at, inputs, diagonal):
    out = lambda n: jax.ShapeDtypeStruct((n, LANES), F32)
    return pl.pallas_call(
        pack_kernel,
        out_shape=(
            out(SEND_B + SEND_E),
            out(SEND_B + SEND_E),
            out(FAR_B + ROWS),
            out(FAR_B + ROWS),
        ),
        in_specs=[SMEM, ANY, VMEM],
        out_specs=(VMEM,) * 4,
        scratch_shapes=[
            pltpu.VMEM((PLANES, 160, LANES), F32),
            pltpu.VMEM((2, COLS, PLANES, 32, LANES), F32),
            pltpu.SemaphoreType.DMA((2,)),
        ],
        compiler_params=pltpu.CompilerParams(vmem_limit_bytes=PACK_LIMIT),
        name="pack",
    )(at, inputs, diagonal)


def prep_kernel(at_ref, src_ref, diag_ref, obs_ref, after_ref, own_ref, probe_ref, edge_ref, win, obs, sems):
    mine = at_ref[0]
    copies = (
        pltpu.make_async_copy(window(src_ref, first_row(mine)), win, sems.at[0]),
        pltpu.make_async_copy(
            obs_ref.at[:, :, pl.ds(pl.multiple_of(mine, 16), ROWS), :], obs, sems.at[1]
        ),
    )
    for c in copies:
        c.start()
    fill_edge(edge_ref, diag_ref)
    for c in copies:
        c.wait()
    flat = win.reshape(COLS * PLANES * 32, LANES)
    seen = obs.reshape(COLS * PLANES * ROWS, LANES)
    for x in range(PLANES):
        offset = x * 32 - first_row(mine)
        turned_rows(own_ref, x * WIDE * COLS, flat, offset, mine - DEPTH, WIDE)
        own_ref[pl.ds(OWN_B + x * 32, 32), :] = edge_ref[x, pl.ds(16 + mine - DEPTH, 32), :]
        for y in range(ROWS):
            v = seen[pl.ds(x * ROWS + y, COLS, stride=PLANES * ROWS), :]
            hi = v.astype(BF16)
            at = pl.ds((x * ROWS + y) * LANES, LANES)
            probe_ref[0:16, at] = hi
            probe_ref[16:32, at] = (v - hi.astype(F32)).astype(BF16)


def prep(at, inputs, diagonal, observations, after):
    return pl.pallas_call(
        prep_kernel,
        out_shape=(
            jax.ShapeDtypeStruct((OWN_B + PLANES * 32, LANES), F32),
            jax.ShapeDtypeStruct((32, PLANES * ROWS * LANES), BF16),
        ),
        in_specs=[SMEM, ANY, VMEM, ANY, ANY],
        out_specs=(VMEM, VMEM),
        scratch_shapes=[
            pltpu.VMEM((PLANES, 160, LANES), F32),
            pltpu.VMEM((COLS, PLANES, 32, LANES), F32),
            pltpu.VMEM((COLS, PLANES, ROWS, LANES), F32),
            pltpu.SemaphoreType.DMA((2,)),
        ],
        compiler_params=pltpu.CompilerParams(vmem_limit_bytes=PACK_LIMIT),
        cost_estimate=pl.CostEstimate(flops=40_000_000, bytes_accessed=4_000_000, transcendentals=0),
        name="prep",
    )(at, inputs, diagonal, observations, after)


def solve_kernel(
    freq_ref, count_ref, own_ref, low_ref, high_ref, low2_ref, high2_ref, probe_ref,
    full_ref, part_ref,
    src, even, odd, near, edge, gre, gim, cat, stage, sems, out_sem,
):
    def start():
        copies = []

        def fetch(a, b):
            copies.append(pltpu.make_async_copy(a, b, sems.at[len(copies)]))
            copies[-1].start()

        fetch(probe_ref, cat.at[pl.ds(64, 32)])
        for x in range(PLANES):
            fetch(
                own_ref.at[pl.ds(x * WIDE * COLS, WIDE * COLS)],
                src.at[DEPTH + x],
            )
        fetch(own_ref.at[pl.ds(OWN_B, PLANES * 32)], stage.at[pl.ds(0, 128)])
        for s, (close, far) in enumerate(((low_ref, low2_ref), (high_ref, high2_ref))):
            base = 0
            for d in range(1, PLANES + 1):
                count = (WIDE - 2 * d) * COLS
                px = DEPTH - d if s == 0 else DEPTH + PLANES - 1 + d
                fetch(close.at[pl.ds(base, count)], src.at[px, pl.ds(d * COLS, count)])
                base += count
            px = 0 if s == 0 else SPAN - 1
            fetch(far.at[pl.ds(0, FAR_B)], src.at[px, pl.ds(DEPTH * COLS, FAR_B)])
            fetch(close.at[pl.ds(SEND_B, SEND_E)], stage.at[pl.ds(128 + s * 112, SEND_E)])
            fetch(far.at[pl.ds(FAR_B, ROWS)], stage.at[pl.ds(128 + s * 112 + 96, ROWS)])
        edge[...] = jnp.zeros_like(edge)
        part_ref[...] = jnp.zeros_like(part_ref)
        apart = lax.broadcasted_iota(jnp.int32, (LANES, LANES), 0) - lax.broadcasted_iota(
            jnp.int32, (LANES, LANES), 1
        )
        ones = jnp.where(jnp.abs(apart) == 1, 1.0, 0.0).astype(BF16)
        near[0:LANES, :] = ones
        near[LANES : 2 * LANES, :] = ones
        for c in copies:
            c.wait()
        for x in range(PLANES):
            edge[DEPTH + x] = stage[pl.ds(x * 32, 32), :]
        for s in range(2):
            for d in range(1, DEPTH + 1):
                px = DEPTH - d if s == 0 else DEPTH + PLANES - 1 + d
                edge[px, pl.ds(d, WIDE - 2 * d), :] = stage[
                    pl.ds(128 + s * 112 + (d - 1) * 24, WIDE - 2 * d), :
                ]

    start()

    @pl.loop(0, QUAD)
    def _(node):
        count = count_ref[node]
        freq = freq_ref[node]

        for px in range(SPAN):
            d = edge[px]
            inv = 1.0 / (d * d + freq * freq)
            gre[px] = d * inv
            gim[px] = jnp.where(d > 0.0, -freq * inv, 0.0)

        def planes(level, top, m, body):
            dd = level - m
            idle = (dd < 0) | (level > top)
            trips = jnp.where(idle, 0, jnp.where(dd == 0, PLANES // 2, 1))

            @pl.loop(0, trips)
            def _(q):
                left = jnp.where(dd == 0, DEPTH + 2 * q, DEPTH - dd)
                right = jnp.where(dd == 0, left + 1, DEPTH + PLANES - 1 + dd)
                body(left, right)

        def spread(ref, px, r):
            return jnp.broadcast_to(ref[px, pl.ds(r, 1), :], (COLS, LANES))

        def at_row(r):
            return pl.ds(r * COLS, COLS)

        def halves(v):
            hi = v.astype(BF16)
            return hi, (v - hi.astype(F32)).astype(BF16)

        def begin(field):
            for m in range(DEPTH + 1):

                def first(*pair_of, m=m):
                    for px in pair_of:
                        for r in range(DEPTH - m, DEPTH + ROWS + m):
                            b = src[px, at_row(r), :]
                            field[0, px, at_row(r), :] = spread(gre, px, r) * b
                            field[1, px, at_row(r), :] = spread(gim, px, r) * b

                planes(count - 1, count - 1, m, first)

        def sweep(old, emit, group, m):
            start, rows = DEPTH - m, ROWS + 2 * m
            beside = []
            for px in group:
                lhs = []
                for i in range(rows):
                    for c in range(2):
                        hi, lo = halves(old[c, px, at_row(start + i), :])
                        lhs.append(jnp.concatenate([hi, lo], 1))
                beside.append(
                    jnp.dot(jnp.concatenate(lhs, 0), near[...], preferred_element_type=F32)
                )
            for px, side in zip(group, beside):

                def get(c, p, r):
                    return old[c, p, at_row(r), :]

                below = [get(c, px, start - 1) for c in range(2)]
                here = [get(c, px, start) for c in range(2)]
                for i in range(rows):
                    r = start + i
                    above = [get(c, px, r + 1) for c in range(2)]
                    re, im = [
                        (get(c, px - 1, r) + get(c, px + 1, r))
                        + (below[c] + above[c])
                        + side[i * 32 + c * COLS : i * 32 + c * COLS + COLS]
                        for c in range(2)
                    ]
                    re = re + src[px, at_row(r), :]
                    p, q = spread(gre, px, r), spread(gim, px, r)
                    emit(px, r, (p * re - q * im, p * im + q * re))
                    below, here = here, above

        @pl.when(lax.rem(count, 2) == 1)
        def _():
            begin(even)

        @pl.when(lax.rem(count, 2) == 0)
        def _():
            begin(odd)

        def into(new):
            def emit(px, r, values):
                for c, v in enumerate(values):
                    new[c, px, at_row(r), :] = v

            return emit

        for level in range(DEPTH - 1, 0, -1):

            @pl.when(level <= count - 2)
            def _(level=level):
                old, new = (odd, even) if level % 2 == 0 else (even, odd)
                sweep(old, into(new), range(DEPTH, DEPTH + PLANES), level)
                for d in range(1, level + 1):
                    sweep(old, into(new), (DEPTH - d, DEPTH + PLANES - 1 + d), level - d)

        leave = pltpu.make_async_copy(
            cat.at[pl.ds(0, 64)],
            full_ref.at[pl.ds(pl.multiple_of(64 * node, 64), 64)],
            out_sem,
        )

        @pl.when(node > 0)
        def _():
            leave.wait()

        def finish(px, r, values):
            at = pl.ds(((px - DEPTH) * ROWS + r - DEPTH) * LANES, LANES)
            for c, v in enumerate(values):
                hi, lo = halves(v)
                cat[pl.ds(c * COLS, COLS), at] = hi
                cat[pl.ds(32 + c * COLS, COLS), at] = lo

        sweep(odd, finish, range(DEPTH, DEPTH + PLANES), 0)
        leave.start()
        o = lax.dot_general(
            cat[...], cat[0:64, :], (((1,), (1,)), ((), ())), preferred_element_type=F32
        )
        o = jnp.concatenate([o, jnp.zeros((96, 64), F32)], 1)
        lane = lax.broadcasted_iota(jnp.int32, (COLS, LANES), 1)
        proj = o[64:80] + pltpu.roll(o[64:80], LANES - 32, 1) + o[80:96]
        proj = pltpu.roll(jnp.where(lane < 32, proj, 0.0), 32 * lax.rem(node, 4), 1)
        part_ref[pl.ds(pl.multiple_of(16 * (node // 4), 16), 16), :] += proj
        gu = o[0:16] + pltpu.roll(o[0:16], LANES - 32, 1) + o[32:48]
        gw = o[16:32] + pltpu.roll(o[16:32], LANES - 32, 1) + o[48:64]
        gram = jnp.where(lane < 16, gu + pltpu.roll(gw, LANES - 16, 1), 0.0)
        part_ref[32:48, :] += pltpu.roll(gram, 16 * node, 1)

    pltpu.make_async_copy(cat.at[pl.ds(0, 64)], full_ref.at[pl.ds(0, 64)], out_sem).wait()


def solve(freqs, counts, own, low, high, low2, high2, probe):
    cells = PLANES * ROWS * LANES
    return pl.pallas_call(
        solve_kernel,
        out_shape=(
            jax.ShapeDtypeStruct((QUAD * 64, cells), BF16),
            jax.ShapeDtypeStruct((48, LANES), F32),
        ),
        in_specs=[SMEM, SMEM] + [ANY] * 6,
        out_specs=(
            pl.BlockSpec(memory_space=pltpu.HBM),
            VMEM,
        ),
        scratch_shapes=[
            pltpu.VMEM((SPAN, WIDE * COLS, LANES), F32),
            pltpu.VMEM((2, SPAN, WIDE * COLS, LANES), F32),
            pltpu.VMEM((2, SPAN, WIDE * COLS, LANES), F32),
            pltpu.VMEM((2 * LANES, LANES), BF16),
            pltpu.VMEM((SPAN, 32, LANES), F32),
            pltpu.VMEM((SPAN, 32, LANES), F32),
            pltpu.VMEM((SPAN, 32, LANES), F32),
            pltpu.VMEM((96, cells), BF16),
            pltpu.VMEM((352, LANES), F32),
            pltpu.SemaphoreType.DMA((24,)),
            pltpu.SemaphoreType.DMA,
        ],
        compiler_params=pltpu.CompilerParams(vmem_limit_bytes=SOLVE_LIMIT),
        name="solve",
    )(freqs, counts, own, low, high, low2, high2, probe)


def respond_kernel(pick_ref, weight_ref, sum_ref, full_ref, out_ref, gram_ref, coef):
    @pl.when(pl.program_id(0) == 0)
    def _():
        lane = lax.broadcasted_iota(jnp.int32, (16, LANES), 1)
        for half in range(2):
            scale = weight_ref[half * 4] * (1.0 / QUAD)
            for j in range(1, 4):
                scale = jnp.where(lane < 32 * j, scale, weight_ref[half * 4 + j] * (1.0 / QUAD))
            acc = sum_ref[16 * half : 16 * half + 16, :] * scale
            for b in range(2):
                one = pltpu.roll(acc, 64, 1) if b else acc
                twice = jnp.where(
                    lane < 32,
                    one,
                    jnp.where(lane < 96, pltpu.roll(one, 32, 1), pltpu.roll(one, 64, 1)),
                )
                at = pl.ds((half * 2 + b) * LANES, LANES)
                hi = twice.astype(BF16)
                coef[0:16, at] = hi
                coef[16:32, at] = (twice - hi.astype(F32)).astype(BF16)
        node = pick_ref[0]
        gram = pltpu.roll(sum_ref[32:48, :], lax.rem(128 - 16 * node, 128), 1)
        gram_ref[...] = gram * (weight_ref[node] * (1.0 / CELLS))

    big = jnp.dot(coef[...], full_ref[...], preferred_element_type=F32)
    res = big[0:16] + big[16:32]
    flat = out_ref.reshape(16 * STEP, LANES)
    for y in range(STEP):
        flat[pl.ds(y, 16, stride=STEP), :] = res[:, y * LANES : (y + 1) * LANES]


def respond(pick, weights, total, full):
    wide = STEP * LANES
    return pl.pallas_call(
        respond_kernel,
        grid=(PLANES * ROWS // STEP,),
        out_shape=(
            jax.ShapeDtypeStruct((16, PLANES, ROWS, LANES), F32),
            jax.ShapeDtypeStruct((16, LANES), F32),
        ),
        in_specs=[
            SMEM,
            SMEM,
            pl.BlockSpec((48, LANES), lambda x: (0, 0)),
            pl.BlockSpec((QUAD * 64, wide), lambda x: (0, x)),
        ],
        out_specs=(
            pl.BlockSpec((16, 1, STEP, LANES), lambda x: (0, x * STEP // ROWS, x % (ROWS // STEP), 0)),
            pl.BlockSpec((16, LANES), lambda x: (0, 0)),
        ),
        scratch_shapes=[pltpu.VMEM((32, QUAD * 64), BF16)],
        compiler_params=pltpu.CompilerParams(
            dimension_semantics=("arbitrary",), vmem_limit_bytes=50 << 20
        ),
        name="respond",
    )(pick, weights, total, full)


def step_pairs(step):
    pairs = []
    for node in range(8):
        for r in range(16):
            t = r + step
            if 0 <= t < 16:
                c, ct = r // 2, t // 2
                flip = c != ct and (c % 2 == 1 if step > 0 else c % 2 == 0)
                pairs.append((node * 16 + r, (node ^ 4 if flip else node) * 16 + t))
    return pairs


def xor_sum(x, axis, size, masks):
    combos = [0]
    for m in masks:
        combos += [c ^ m for c in combos]
    got = [x if c == 0 else lax.ppermute(x, axis, [(i, i ^ c) for i in range(size)]) for c in combos]
    while len(got) > 1:
        got = [got[i] + got[i + 1] for i in range(0, len(got), 2)]
    return got[0]


def turn(v, by):
    return lax.ppermute(v, "node", [(i, i // 4 * 4 + (i + by) % 4) for i in range(8)])


def across(v):
    return lax.ppermute(v, "node", [(i, i ^ 4) for i in range(8)])


def place_kernel(spot_ref, *refs):
    pieces, out_ref, sems = refs[:10], refs[10], refs[11]
    copies = []
    for g in range(2):
        for k, (slot, first) in enumerate(((0, 0), (1, 0), (2, 0), (3, 0), (3, 8))):
            piece = pieces[g * 5 + k]
            at = pl.multiple_of(spot_ref[g * 4 + slot], ROWS)
            dst = out_ref.at[pl.ds(first, piece.shape[0]), :, pl.ds(at, ROWS), :]
            copies.append(pltpu.make_async_copy(piece, dst, sems.at[g * 5 + k]))
    for c in copies:
        c.start()
    for c in copies:
        c.wait()


def place(spots, pieces):
    return pl.pallas_call(
        place_kernel,
        out_shape=jax.ShapeDtypeStruct((16, PLANES, 128, LANES), F32),
        in_specs=[SMEM] + [VMEM] * 10,
        out_specs=pl.BlockSpec(memory_space=pltpu.HBM),
        scratch_shapes=[pltpu.SemaphoreType.DMA((10,))],
        compiler_params=pltpu.CompilerParams(vmem_limit_bytes=8 << 20),
        name="place",
    )(spots, *pieces)


def local(inputs, diagonal, observations, frequencies, weights, counts, assignment):
    node = lax.axis_index("node")
    row = lax.axis_index("row")
    core, odd = row % 2, (row // 2) % 2
    fwd2 = node ^ (4 * odd)
    bwd2 = node ^ (4 * (1 - odd))
    fwd = jnp.where(core == 1, fwd2, node)
    bwd = jnp.where(core == 0, bwd2, node)
    at = (16 * jnp.stack([node, fwd, bwd, fwd2, bwd2])).astype(jnp.int32)
    s1, s2, s3, s4 = pack(at, inputs, diagonal)
    own, probe = prep(at, inputs, diagonal, observations, s3)
    both = ("node", "row")
    low = lax.ppermute(s1, both, step_pairs(1))
    high = lax.ppermute(s2, both, step_pairs(-1))
    low2 = lax.ppermute(s3, both, step_pairs(2))
    high2 = lax.ppermute(s4, both, step_pairs(-2))
    fields, part = solve(frequencies, counts, own, low, high, low2, high2, probe)
    total = xor_sum(part, "row", 16, [1, 2])
    total = xor_sum(total, "row", 16, [4, 8])
    total = xor_sum(total, "node", 8, [1, 2])
    total = xor_sum(total, "node", 8, [4])
    pick = lax.dynamic_slice_in_dim(assignment, node, 1)
    mine, gram = respond(pick, weights, total, fields)

    left, right, other = turn(mine, 1), turn(mine, -1), across(mine)
    far0, far1 = turn(left[:8], 1), turn(right[8:], -1)
    left_o, right_o = turn(other, 1), turn(other, -1)
    far0_o, far1_o = across(far0), across(far1)
    x, z = node % 4, node // 4
    spots = []
    for side in (z, 1 - z):
        spots += [(side * 4 + (x + dx) % 4) * ROWS for dx in (0, 3, 1, 2)]
    full = place(
        jnp.stack(spots).astype(jnp.int32),
        (mine, left, right, far0, far1, other, left_o, right_o, far0_o, far1_o),
    )
    return full, gram[None, :, :16]


def solution(mesh):
    placed = (
        P(None, "row", None, None),
        P("row", None, None),
        P(None, "row", None, None),
        P(),
        P(),
        P(),
        P(),
    )
    return jax.shard_map(
        local,
        mesh=mesh,
        in_specs=placed,
        out_specs=(P(None, "row", None, None), P("node", None, None)),
        check_vma=False,
    )
```

```python
import jax
import jax.numpy as jnp
from jax import lax
from jax.experimental import pallas as pl
from jax.experimental.pallas import tpu as pltpu
from jax.sharding import PartitionSpec as P

QUAD = 8
COLS = 16
DEPTH = 5
PLANES = 4
ROWS = 16
WIDE = ROWS + 2 * DEPTH
SPAN = PLANES + 2 * DEPTH
LANES = 128
CELLS = 1048576.0
SEND_B = sum(WIDE - 2 * d for d in range(1, PLANES + 1)) * COLS
SEND_E = PLANES * 24
FAR_B = ROWS * COLS
OWN_B = PLANES * WIDE * COLS
STEP = 8
PART = 2048
PACK_LIMIT = 50 << 20
SOLVE_LIMIT = 51 << 20
F32 = jnp.float32
BF16 = jnp.bfloat16
VMEM = pl.BlockSpec(memory_space=pltpu.VMEM)
SMEM = pl.BlockSpec(memory_space=pltpu.SMEM)
ANY = pl.BlockSpec(memory_space=pl.ANY)


def window_copies(src_ref, start, dst_ref, sems):
    rows = pl.ds(pl.multiple_of(start, 8), 32)
    return [
        pltpu.make_async_copy(
            src_ref.at[pl.ds(2 * i, 2), :, rows, :], dst_ref.at[pl.ds(2 * i, 2)], sems.at[i]
        )
        for i in range(COLS // 2)
    ]


def first_row(at):
    return jnp.clip(at - 8, 0, 96)


def fill_edge(edge_ref, diag_ref):
    for x in range(PLANES):
        edge_ref[x, pl.ds(0, 16), :] = jnp.zeros((16, LANES), F32)
        edge_ref[x, pl.ds(144, 16), :] = jnp.zeros((16, LANES), F32)
        edge_ref[x, pl.ds(16, 128), :] = diag_ref[x] + 6.0


def turned_rows(dst_ref, base, flat_ref, offset, first, count):
    for q in range(count):
        y = jnp.clip(first + q, 0, 127) + offset
        dst_ref[pl.ds(base + q * COLS, COLS), :] = flat_ref[
            pl.ds(y, COLS, stride=PLANES * 32), :
        ]


def pack_kernel(
    at_ref, src_ref, diag_hbm, fwd_ref, bwd_ref, fwd2_ref, bwd2_ref, edge_ref, diag_ref, win, sems
):
    mine = at_ref[0]
    other = jnp.where(mine >= 64, mine - 64, mine + 64)
    whole = pltpu.make_async_copy(diag_hbm, diag_ref, sems.at[2, 0])
    whole.start()
    copies = []
    for w, t in enumerate((mine, other)):
        copies += window_copies(src_ref, first_row(t), win.at[w], sems.at[w])
    for c in copies:
        c.start()
    whole.wait()
    fill_edge(edge_ref, diag_ref)
    for c in copies:
        c.wait()
    flat = win.reshape(2 * COLS * PLANES * 32, LANES)

    def send(dst_ref, base, at, plane, d, count):
        offset = jnp.where(at == mine, 0, COLS * PLANES * 32) + plane * 32 - first_row(at)
        turned_rows(dst_ref, base, flat, offset, at - DEPTH + d, count)

    base = 0
    for d in range(1, PLANES + 1):
        count = WIDE - 2 * d
        for dst_ref, at, plane in ((fwd_ref, at_ref[1], PLANES - d), (bwd_ref, at_ref[2], d - 1)):
            send(dst_ref, base, at, plane, d, count)
            dst_ref[pl.ds(SEND_B + (d - 1) * 24, 24), :] = edge_ref[
                plane, pl.ds(16 + at - DEPTH + d, 24), :
            ]
        base += count * COLS
    for dst_ref, at, plane in ((fwd2_ref, at_ref[3], PLANES - 1), (bwd2_ref, at_ref[4], 0)):
        send(dst_ref, 0, at, plane, DEPTH, ROWS)
        dst_ref[pl.ds(FAR_B, ROWS), :] = edge_ref[plane, pl.ds(16 + at, ROWS), :]


def pack(at, inputs, diagonal):
    out = lambda n: jax.ShapeDtypeStruct((n, LANES), F32)
    return pl.pallas_call(
        pack_kernel,
        out_shape=(
            out(SEND_B + SEND_E),
            out(SEND_B + SEND_E),
            out(FAR_B + ROWS),
            out(FAR_B + ROWS),
        ),
        in_specs=[SMEM, ANY, ANY],
        out_specs=(VMEM,) * 4,
        scratch_shapes=[
            pltpu.VMEM((PLANES, 160, LANES), F32),
            pltpu.VMEM((PLANES, 128, LANES), F32),
            pltpu.VMEM((2, COLS, PLANES, 32, LANES), F32),
            pltpu.SemaphoreType.DMA((3, 8)),
        ],
        compiler_params=pltpu.CompilerParams(vmem_limit_bytes=PACK_LIMIT),
        name="pack",
    )(at, inputs, diagonal)


def prep_kernel(at_ref, src_ref, diag_ref, obs_ref, after_ref, own_ref, probe_ref, edge_ref, win, obs, sems):
    mine = at_ref[0]
    copies = window_copies(src_ref, first_row(mine), win, sems)
    copies.append(
        pltpu.make_async_copy(
            obs_ref.at[:, :, pl.ds(pl.multiple_of(mine, 16), ROWS), :], obs, sems.at[8]
        )
    )
    for c in copies:
        c.start()
    fill_edge(edge_ref, diag_ref)
    for c in copies:
        c.wait()
    flat = win.reshape(COLS * PLANES * 32, LANES)
    seen = obs.reshape(COLS * PLANES * ROWS, LANES)
    for x in range(PLANES):
        offset = x * 32 - first_row(mine)
        turned_rows(own_ref, x * WIDE * COLS, flat, offset, mine - DEPTH, WIDE)
        own_ref[pl.ds(OWN_B + x * 32, 32), :] = edge_ref[x, pl.ds(16 + mine - DEPTH, 32), :]
        for y in range(ROWS):
            v = seen[pl.ds(x * ROWS + y, COLS, stride=PLANES * ROWS), :]
            hi = v.astype(BF16)
            at = pl.ds((x * ROWS + y) * LANES, LANES)
            probe_ref[0:16, at] = hi
            probe_ref[16:32, at] = (v - hi.astype(F32)).astype(BF16)


def prep(at, inputs, diagonal, observations, after):
    return pl.pallas_call(
        prep_kernel,
        out_shape=(
            jax.ShapeDtypeStruct((OWN_B + PLANES * 32, LANES), F32),
            jax.ShapeDtypeStruct((32, PLANES * ROWS * LANES), BF16),
        ),
        in_specs=[SMEM, ANY, VMEM, ANY, ANY],
        out_specs=(VMEM, VMEM),
        scratch_shapes=[
            pltpu.VMEM((PLANES, 160, LANES), F32),
            pltpu.VMEM((COLS, PLANES, 32, LANES), F32),
            pltpu.VMEM((COLS, PLANES, ROWS, LANES), F32),
            pltpu.SemaphoreType.DMA((9,)),
        ],
        compiler_params=pltpu.CompilerParams(vmem_limit_bytes=PACK_LIMIT),
        cost_estimate=pl.CostEstimate(flops=40_000_000, bytes_accessed=4_000_000, transcendentals=0),
        name="prep",
    )(at, inputs, diagonal, observations, after)


def solve_kernel(
    freq_ref, count_ref, own_ref, low_ref, high_ref, low2_ref, high2_ref, probe_ref,
    full_ref, part_ref,
    src, even, odd, near, edge, gre, gim, cat, stage, sems, out_sem,
):
    def start():
        copies = []

        def fetch(a, b):
            copies.append(pltpu.make_async_copy(a, b, sems.at[len(copies)]))
            copies[-1].start()

        fetch(probe_ref, cat.at[pl.ds(64, 32)])
        for x in range(PLANES):
            fetch(
                own_ref.at[pl.ds(x * WIDE * COLS, WIDE * COLS)],
                src.at[DEPTH + x],
            )
        fetch(own_ref.at[pl.ds(OWN_B, PLANES * 32)], stage.at[pl.ds(0, 128)])
        for s, (close, far) in enumerate(((low_ref, low2_ref), (high_ref, high2_ref))):
            base = 0
            for d in range(1, PLANES + 1):
                count = (WIDE - 2 * d) * COLS
                px = DEPTH - d if s == 0 else DEPTH + PLANES - 1 + d
                fetch(close.at[pl.ds(base, count)], src.at[px, pl.ds(d * COLS, count)])
                base += count
            px = 0 if s == 0 else SPAN - 1
            fetch(far.at[pl.ds(0, FAR_B)], src.at[px, pl.ds(DEPTH * COLS, FAR_B)])
            fetch(close.at[pl.ds(SEND_B, SEND_E)], stage.at[pl.ds(128 + s * 112, SEND_E)])
            fetch(far.at[pl.ds(FAR_B, ROWS)], stage.at[pl.ds(128 + s * 112 + 96, ROWS)])
        edge[...] = jnp.zeros_like(edge)
        part_ref[...] = jnp.zeros_like(part_ref)
        apart = lax.broadcasted_iota(jnp.int32, (LANES, LANES), 0) - lax.broadcasted_iota(
            jnp.int32, (LANES, LANES), 1
        )
        ones = jnp.where(jnp.abs(apart) == 1, 1.0, 0.0).astype(BF16)
        near[0:LANES, :] = ones
        near[LANES : 2 * LANES, :] = ones
        for c in copies:
            c.wait()
        for x in range(PLANES):
            edge[DEPTH + x] = stage[pl.ds(x * 32, 32), :]
        for s in range(2):
            for d in range(1, DEPTH + 1):
                px = DEPTH - d if s == 0 else DEPTH + PLANES - 1 + d
                edge[px, pl.ds(d, WIDE - 2 * d), :] = stage[
                    pl.ds(128 + s * 112 + (d - 1) * 24, WIDE - 2 * d), :
                ]

    def leaving(node):
        return [
            pltpu.make_async_copy(
                cat.at[pl.ds(64 * i, 64)],
                full_ref.at[pl.ds(pl.multiple_of(64 * node + 64 * i, 8), 64)],
                out_sem.at[i],
            )
            for i in range(1)
        ]

    start()

    @pl.loop(0, QUAD)
    def _(node):
        count = count_ref[node]
        freq = freq_ref[node]

        for px in range(SPAN):
            d = edge[px]
            inv = 1.0 / (d * d + freq * freq)
            gre[px] = d * inv
            gim[px] = jnp.where(d > 0.0, -freq * inv, 0.0)

        def planes(level, top, m, body):
            dd = level - m
            idle = (dd < 0) | (level > top)
            trips = jnp.where(idle, 0, jnp.where(dd == 0, PLANES // 2, 1))

            @pl.loop(0, trips)
            def _(q):
                left = jnp.where(dd == 0, DEPTH + 2 * q, DEPTH - dd)
                right = jnp.where(dd == 0, left + 1, DEPTH + PLANES - 1 + dd)
                body(left, right)

        def spread(ref, px, r):
            return jnp.broadcast_to(ref[px, pl.ds(r, 1), :], (COLS, LANES))

        def at_row(r):
            return pl.ds(r * COLS, COLS)

        def halves(v):
            hi = v.astype(BF16)
            return hi, (v - hi.astype(F32)).astype(BF16)

        def begin(field):
            for m in range(DEPTH + 1):

                def first(*pair_of, m=m):
                    for px in pair_of:
                        for r in range(DEPTH - m, DEPTH + ROWS + m):
                            b = src[px, at_row(r), :]
                            field[0, px, at_row(r), :] = spread(gre, px, r) * b
                            field[1, px, at_row(r), :] = spread(gim, px, r) * b

                planes(count - 1, count - 1, m, first)

        def sweep(old, emit, group, m):
            start, rows = DEPTH - m, ROWS + 2 * m
            beside = []
            for px in group:
                lhs = []
                for i in range(rows):
                    for c in range(2):
                        hi, lo = halves(old[c, px, at_row(start + i), :])
                        lhs.append(jnp.concatenate([hi, lo], 1))
                beside.append(
                    jnp.dot(jnp.concatenate(lhs, 0), near[...], preferred_element_type=F32)
                )
            for px, side in zip(group, beside):

                def get(c, p, r):
                    return old[c, p, at_row(r), :]

                below = [get(c, px, start - 1) for c in range(2)]
                here = [get(c, px, start) for c in range(2)]
                for i in range(rows):
                    r = start + i
                    above = [get(c, px, r + 1) for c in range(2)]
                    re, im = [
                        (get(c, px - 1, r) + get(c, px + 1, r))
                        + (below[c] + above[c])
                        + side[i * 32 + c * COLS : i * 32 + c * COLS + COLS]
                        for c in range(2)
                    ]
                    re = re + src[px, at_row(r), :]
                    p, q = spread(gre, px, r), spread(gim, px, r)
                    emit(px, r, (p * re - q * im, p * im + q * re))
                    below, here = here, above

        @pl.when(lax.rem(count, 2) == 1)
        def _():
            begin(even)

        @pl.when(lax.rem(count, 2) == 0)
        def _():
            begin(odd)

        def into(new):
            def emit(px, r, values):
                for c, v in enumerate(values):
                    new[c, px, at_row(r), :] = v

            return emit

        for level in range(DEPTH - 1, 0, -1):

            @pl.when(level <= count - 2)
            def _(level=level):
                old, new = (odd, even) if level % 2 == 0 else (even, odd)
                sweep(old, into(new), range(DEPTH, DEPTH + PLANES), level)
                for d in range(1, level + 1):
                    sweep(old, into(new), (DEPTH - d, DEPTH + PLANES - 1 + d), level - d)

        leave = leaving(node)

        @pl.when(node > 0)
        def _():
            for c in leave:
                c.wait()

        def finish(px, r, values):
            at = pl.ds(((px - DEPTH) * ROWS + r - DEPTH) * LANES, LANES)
            for c, v in enumerate(values):
                hi, lo = halves(v)
                cat[pl.ds(32 + c * COLS, COLS), at] = hi
                cat[pl.ds(c * COLS, COLS), at] = lo

        sweep(odd, finish, range(DEPTH, DEPTH + PLANES), 0)
        for c in leave:
            c.start()
        o = lax.dot_general(
            cat[32:96, :], cat[0:64, :], (((1,), (1,)), ((), ())), preferred_element_type=F32
        )
        o = jnp.concatenate([o, jnp.zeros((64, 64), F32)], 1)
        lane = lax.broadcasted_iota(jnp.int32, (COLS, LANES), 1)
        seen = o[32:48] + o[48:64]
        proj = seen + pltpu.roll(seen, LANES - 32, 1)
        proj = pltpu.roll(jnp.where(lane < 32, proj, 0.0), 32 * lax.rem(node, 4), 1)
        part_ref[pl.ds(pl.multiple_of(16 * (node // 4), 16), 16), :] += proj
        half = o[0:32] + 0.5 * pltpu.roll(o[0:32], LANES - 32, 1)
        gram = half[0:16] + pltpu.roll(half[16:32], LANES - 16, 1)
        gram = jnp.where(lane < 16, gram, 0.0)
        part_ref[32:48, :] += pltpu.roll(gram, 16 * node, 1)

    for c in leaving(0):
        c.wait()


def solve(freqs, counts, own, low, high, low2, high2, probe):
    cells = PLANES * ROWS * LANES
    return pl.pallas_call(
        solve_kernel,
        out_shape=(
            jax.ShapeDtypeStruct((QUAD * 64, cells), BF16),
            jax.ShapeDtypeStruct((48, LANES), F32),
        ),
        in_specs=[SMEM, SMEM] + [ANY] * 6,
        out_specs=(
            pl.BlockSpec(memory_space=pltpu.HBM),
            VMEM,
        ),
        scratch_shapes=[
            pltpu.VMEM((SPAN, WIDE * COLS, LANES), F32),
            pltpu.VMEM((2, SPAN, WIDE * COLS, LANES), F32),
            pltpu.VMEM((2, SPAN, WIDE * COLS, LANES), F32),
            pltpu.VMEM((2 * LANES, LANES), BF16),
            pltpu.VMEM((SPAN, 32, LANES), F32),
            pltpu.VMEM((SPAN, 32, LANES), F32),
            pltpu.VMEM((SPAN, 32, LANES), F32),
            pltpu.VMEM((96, cells), BF16),
            pltpu.VMEM((352, LANES), F32),
            pltpu.SemaphoreType.DMA((24,)),
            pltpu.SemaphoreType.DMA((8,)),
        ],
        compiler_params=pltpu.CompilerParams(vmem_limit_bytes=SOLVE_LIMIT),
        name="solve",
    )(freqs, counts, own, low, high, low2, high2, probe)


def respond_kernel(pick_ref, weight_ref, sum_ref, full_ref, out_ref, gram_ref, coef, full, sems):
    parts = PLANES * ROWS // STEP
    wide = STEP * LANES
    copies = [
        [
            pltpu.make_async_copy(
                full_ref.at[pl.ds(128 * j, 128), pl.ds(t * wide, wide)],
                full.at[t, pl.ds(128 * j, 128), :],
                sems.at[t, j],
            )
            for j in range(4)
        ]
        for t in range(parts)
    ]
    for group in copies:
        for c in group:
            c.start()
    lane = lax.broadcasted_iota(jnp.int32, (16, LANES), 1)
    for half in range(2):
        scale = weight_ref[half * 4] * (1.0 / QUAD)
        for j in range(1, 4):
            scale = jnp.where(lane < 32 * j, scale, weight_ref[half * 4 + j] * (1.0 / QUAD))
        acc = sum_ref[16 * half : 16 * half + 16, :] * scale
        for b in range(2):
            one = pltpu.roll(acc, 64, 1) if b else acc
            twice = jnp.where(
                lane < 32,
                one,
                jnp.where(lane < 96, pltpu.roll(one, 32, 1), pltpu.roll(one, 64, 1)),
            )
            at = pl.ds((half * 2 + b) * LANES, LANES)
            hi = twice.astype(BF16)
            coef[0:16, at] = hi
            coef[16:32, at] = (twice - hi.astype(F32)).astype(BF16)
    node = pick_ref[0]
    gram = pltpu.roll(sum_ref[32:48, :], lax.rem(128 - 16 * node, 128), 1)
    gram = gram * (weight_ref[node] * (1.0 / CELLS))
    gram_ref[:, 0:16] = gram[:, 0:16] + gram.T[0:16, :]

    flat = out_ref.reshape(16 * PLANES * ROWS, LANES)
    for t, group in enumerate(copies):
        for c in group:
            c.wait()
        big = jnp.dot(coef[...], full[t], preferred_element_type=F32)
        res = big[0:16] + big[16:32]
        for y in range(STEP):
            flat[pl.ds(t * STEP + y, 16, stride=PLANES * ROWS), :] = res[
                :, y * LANES : (y + 1) * LANES
            ]


def respond(pick, weights, total, full):
    parts = PLANES * ROWS // STEP
    return pl.pallas_call(
        respond_kernel,
        out_shape=(
            jax.ShapeDtypeStruct((16, PLANES, ROWS, LANES), F32),
            jax.ShapeDtypeStruct((16, LANES), F32),
        ),
        in_specs=[SMEM, SMEM, VMEM, ANY],
        out_specs=(VMEM, VMEM),
        scratch_shapes=[
            pltpu.VMEM((32, QUAD * 64), BF16),
            pltpu.VMEM((parts, QUAD * 64, STEP * LANES), BF16),
            pltpu.SemaphoreType.DMA((parts, 4)),
        ],
        compiler_params=pltpu.CompilerParams(vmem_limit_bytes=50 << 20),
        name="respond",
    )(pick, weights, total, full)


def step_pairs(step):
    pairs = []
    for node in range(8):
        for r in range(16):
            t = r + step
            if 0 <= t < 16:
                c, ct = r // 2, t // 2
                flip = c != ct and (c % 2 == 1 if step > 0 else c % 2 == 0)
                pairs.append((node * 16 + r, (node ^ 4 if flip else node) * 16 + t))
    return pairs


def xor_sum(x, axis, size, masks):
    combos = [0]
    for m in masks:
        combos += [c ^ m for c in combos]
    got = [x if c == 0 else lax.ppermute(x, axis, [(i, i ^ c) for i in range(size)]) for c in combos]
    while len(got) > 1:
        got = [got[i] + got[i + 1] for i in range(0, len(got), 2)]
    return got[0]


def turn(v, by):
    return lax.ppermute(v, "node", [(i, i // 4 * 4 + (i + by) % 4) for i in range(8)])


def across(v):
    return lax.ppermute(v, "node", [(i, i ^ 4) for i in range(8)])


def place_into(out_ref, spot_ref, pieces, spots, sems):
    copies = []
    for piece, (slot, first) in zip(pieces, spots):
        at = pl.multiple_of(spot_ref[slot], ROWS)
        for i in range(0, piece.shape[0], 4):
            dst = out_ref.at[pl.ds(first + i, 4), :, pl.ds(at, ROWS), :]
            copies.append(pltpu.make_async_copy(piece.at[pl.ds(i, 4)], dst, sems.at[len(copies)]))
    for c in copies:
        c.start()
    for c in copies:
        c.wait()


EARLY = ((0, 0), (1, 0), (2, 0), (4, 0), (3, 0), (3, 8))
LATE = ((5, 0), (6, 0), (7, 0), (7, 8))


def early_kernel(spot_ref, *refs):
    place_into(refs[6], spot_ref, refs[:6], EARLY, refs[7])


def late_kernel(spot_ref, *refs):
    place_into(refs[5], spot_ref, refs[:4], LATE, refs[6])


def place(spots, early, late):
    whole = jax.ShapeDtypeStruct((16, PLANES, 128, LANES), F32)
    params = pltpu.CompilerParams(vmem_limit_bytes=50 << 20)
    begun = pl.pallas_call(
        early_kernel,
        out_shape=whole,
        in_specs=[SMEM] + [VMEM] * 6,
        out_specs=ANY,
        scratch_shapes=[pltpu.SemaphoreType.DMA((20,))],
        compiler_params=params,
        name="early",
    )(spots, *early)
    return pl.pallas_call(
        late_kernel,
        out_shape=whole,
        in_specs=[SMEM] + [VMEM] * 4 + [ANY],
        out_specs=ANY,
        scratch_shapes=[pltpu.SemaphoreType.DMA((12,))],
        input_output_aliases={5: 0},
        compiler_params=params,
        name="late",
    )(spots, *late, begun)


def local(inputs, diagonal, observations, frequencies, weights, counts, assignment):
    node = lax.axis_index("node")
    row = lax.axis_index("row")
    core, odd = row % 2, (row // 2) % 2
    fwd2 = node ^ (4 * odd)
    bwd2 = node ^ (4 * (1 - odd))
    fwd = jnp.where(core == 1, fwd2, node)
    bwd = jnp.where(core == 0, bwd2, node)
    at = (16 * jnp.stack([node, fwd, bwd, fwd2, bwd2])).astype(jnp.int32)
    s1, s2, s3, s4 = pack(at, inputs, diagonal)
    own, probe = prep(at, inputs, diagonal, observations, s3)
    both = ("node", "row")
    low = lax.ppermute(s1, both, step_pairs(1))
    high = lax.ppermute(s2, both, step_pairs(-1))
    low2 = lax.ppermute(s3, both, step_pairs(2))
    high2 = lax.ppermute(s4, both, step_pairs(-2))
    fields, part = solve(frequencies, counts, own, low, high, low2, high2, probe)
    total = xor_sum(part, "row", 16, [1, 2])
    total = xor_sum(total, "row", 16, [4, 8])
    total = xor_sum(total, "node", 8, [1, 2])
    total = xor_sum(total, "node", 8, [4])
    pick = lax.dynamic_slice_in_dim(assignment, node, 1)
    mine, gram = respond(pick, weights, total, fields)

    left, right, other = turn(mine, 1), turn(mine, -1), across(mine)
    far0, far1 = turn(left[:8], 1), turn(right[8:], -1)
    left_o, right_o = turn(other, 1), turn(other, -1)
    far0_o, far1_o = across(far0), across(far1)
    x, z = node % 4, node // 4
    spots = []
    for side in (z, 1 - z):
        spots += [(side * 4 + (x + dx) % 4) * ROWS for dx in (0, 3, 1, 2)]
    full = place(
        jnp.stack(spots).astype(jnp.int32),
        (mine, left, right, other, far0, far1),
        (left_o, right_o, far0_o, far1_o),
    )
    return full, gram[None, :, :16]


def solution(mesh):
    placed = (
        P(None, "row", None, None),
        P("row", None, None),
        P(None, "row", None, None),
        P(),
        P(),
        P(),
        P(),
    )
    return jax.shard_map(
        local,
        mesh=mesh,
        in_specs=placed,
        out_specs=(P(None, "row", None, None), P("node", None, None)),
        check_vma=False,
    )
```

```python
import jax
import jax.numpy as jnp
from jax import lax
from jax.experimental import pallas as pl
from jax.experimental.pallas import tpu as pltpu
from jax.sharding import PartitionSpec as P

QUAD = 8
COLS = 16
DEPTH = 5
PLANES = 4
ROWS = 16
WIDE = ROWS + 2 * DEPTH
SPAN = PLANES + 2 * DEPTH
LANES = 128
CELLS = 1048576.0
SEND_B = sum(WIDE - 2 * d for d in range(1, PLANES + 1)) * COLS
SEND_E = PLANES * 24
FAR_B = ROWS * COLS
OWN_B = PLANES * WIDE * COLS
STEP = 8
PART = 2048
PACK_LIMIT = 50 << 20
SOLVE_LIMIT = 51 << 20
F32 = jnp.float32
BF16 = jnp.bfloat16
VMEM = pl.BlockSpec(memory_space=pltpu.VMEM)
SMEM = pl.BlockSpec(memory_space=pltpu.SMEM)
ANY = pl.BlockSpec(memory_space=pl.ANY)


def window_copies(src_ref, start, dst_ref, sems):
    rows = pl.ds(pl.multiple_of(start, 8), 32)
    return [
        pltpu.make_async_copy(
            src_ref.at[pl.ds(2 * i, 2), :, rows, :], dst_ref.at[pl.ds(2 * i, 2)], sems.at[i]
        )
        for i in range(COLS // 2)
    ]


def first_row(at):
    return jnp.clip(at - 8, 0, 96)


def fill_edge(edge_ref, diag_ref):
    for x in range(PLANES):
        edge_ref[x, pl.ds(0, 16), :] = jnp.zeros((16, LANES), F32)
        edge_ref[x, pl.ds(144, 16), :] = jnp.zeros((16, LANES), F32)
        edge_ref[x, pl.ds(16, 128), :] = diag_ref[x] + 6.0


def turned_rows(dst_ref, base, flat_ref, offset, first, count):
    for q in range(count):
        y = jnp.clip(first + q, 0, 127) + offset
        dst_ref[pl.ds(base + q * COLS, COLS), :] = flat_ref[
            pl.ds(y, COLS, stride=PLANES * 32), :
        ]


def pack_kernel(
    at_ref, src_ref, diag_hbm, pair_ref, cross_ref, even_ref, odd_ref, edge_ref, diag_ref, win, sems
):
    mine = at_ref[0]
    other = jnp.where(mine >= 64, mine - 64, mine + 64)
    whole = pltpu.make_async_copy(diag_hbm, diag_ref, sems.at[2, 0])
    whole.start()
    copies = []
    for w, t in enumerate((mine, other)):
        copies += window_copies(src_ref, first_row(t), win.at[w], sems.at[w])
    for c in copies:
        c.start()
    whole.wait()
    fill_edge(edge_ref, diag_ref)
    for c in copies:
        c.wait()
    flat = win.reshape(2 * COLS * PLANES * 32, LANES)

    def send(dst_ref, base, at, plane, d, count):
        offset = jnp.where(at == mine, 0, COLS * PLANES * 32) + plane * 32 - first_row(at)
        turned_rows(dst_ref, base, flat, offset, at - DEPTH + d, count)

    core, odd = at_ref[2], at_ref[3]
    base = 0
    for d in range(1, PLANES + 1):
        count = WIDE - 2 * d
        for dst_ref, at, right in ((pair_ref, mine, core == 0), (cross_ref, at_ref[1], core == 1)):
            plane = jnp.where(right, PLANES - d, d - 1)
            send(dst_ref, base, at, plane, d, count)
            dst_ref[pl.ds(SEND_B + (d - 1) * 24, 24), :] = edge_ref[
                plane, pl.ds(16 + at - DEPTH + d, 24), :
            ]
        base += count * COLS
    for dst_ref, at, right in ((even_ref, mine, odd == 0), (odd_ref, other, odd == 1)):
        plane = jnp.where(right, PLANES - 1, 0)
        send(dst_ref, 0, at, plane, DEPTH, ROWS)
        dst_ref[pl.ds(FAR_B, ROWS), :] = edge_ref[plane, pl.ds(16 + at, ROWS), :]


def pack(at, inputs, diagonal):
    out = lambda n: jax.ShapeDtypeStruct((n, LANES), F32)
    return pl.pallas_call(
        pack_kernel,
        out_shape=(
            out(SEND_B + SEND_E),
            out(SEND_B + SEND_E),
            out(FAR_B + ROWS),
            out(FAR_B + ROWS),
        ),
        in_specs=[SMEM, ANY, ANY],
        out_specs=(VMEM,) * 4,
        scratch_shapes=[
            pltpu.VMEM((PLANES, 160, LANES), F32),
            pltpu.VMEM((PLANES, 128, LANES), F32),
            pltpu.VMEM((2, COLS, PLANES, 32, LANES), F32),
            pltpu.SemaphoreType.DMA((3, 8)),
        ],
        compiler_params=pltpu.CompilerParams(vmem_limit_bytes=PACK_LIMIT),
        name="pack",
    )(at, inputs, diagonal)


def prep_kernel(at_ref, src_ref, diag_ref, obs_ref, after_ref, own_ref, probe_ref, edge_ref, win, obs, sems):
    mine = at_ref[0]
    copies = window_copies(src_ref, first_row(mine), win, sems)
    copies.append(
        pltpu.make_async_copy(
            obs_ref.at[:, :, pl.ds(pl.multiple_of(mine, 16), ROWS), :], obs, sems.at[8]
        )
    )
    for c in copies:
        c.start()
    fill_edge(edge_ref, diag_ref)
    for c in copies:
        c.wait()
    flat = win.reshape(COLS * PLANES * 32, LANES)
    seen = obs.reshape(COLS * PLANES * ROWS, LANES)
    for x in range(PLANES):
        offset = x * 32 - first_row(mine)
        turned_rows(own_ref, x * WIDE * COLS, flat, offset, mine - DEPTH, WIDE)
        own_ref[pl.ds(OWN_B + x * 32, 32), :] = edge_ref[x, pl.ds(16 + mine - DEPTH, 32), :]
        for y in range(ROWS):
            v = seen[pl.ds(x * ROWS + y, COLS, stride=PLANES * ROWS), :]
            hi = v.astype(BF16)
            at = pl.ds((x * ROWS + y) * LANES, LANES)
            probe_ref[0:16, at] = hi
            probe_ref[16:32, at] = (v - hi.astype(F32)).astype(BF16)


def prep(at, inputs, diagonal, observations, after):
    return pl.pallas_call(
        prep_kernel,
        out_shape=(
            jax.ShapeDtypeStruct((OWN_B + PLANES * 32, LANES), F32),
            jax.ShapeDtypeStruct((32, PLANES * ROWS * LANES), BF16),
        ),
        in_specs=[SMEM, ANY, VMEM, ANY, ANY],
        out_specs=(VMEM, VMEM),
        scratch_shapes=[
            pltpu.VMEM((PLANES, 160, LANES), F32),
            pltpu.VMEM((COLS, PLANES, 32, LANES), F32),
            pltpu.VMEM((COLS, PLANES, ROWS, LANES), F32),
            pltpu.SemaphoreType.DMA((9,)),
        ],
        compiler_params=pltpu.CompilerParams(vmem_limit_bytes=PACK_LIMIT),
        cost_estimate=pl.CostEstimate(flops=40_000_000, bytes_accessed=4_000_000, transcendentals=0),
        name="prep",
    )(at, inputs, diagonal, observations, after)


def solve_kernel(
    at_ref, freq_ref, count_ref, own_ref, pair_ref, cross_ref, even_ref, odd_ref, probe_ref,
    full_ref, part_ref,
    src, even, odd, near, edge, gre, gim, cat, stage, sems, out_sem,
):
    core, half_odd = at_ref[2], at_ref[3]

    def ghost(s, d):
        if d < DEPTH:
            right = core == s
        else:
            right = half_odd == s
        return jnp.where(right, DEPTH + PLANES - 1 + d, DEPTH - d)

    def start():
        copies = []

        def fetch(a, b):
            copies.append(pltpu.make_async_copy(a, b, sems.at[len(copies)]))
            copies[-1].start()

        fetch(probe_ref, cat.at[pl.ds(64, 32)])
        for x in range(PLANES):
            fetch(
                own_ref.at[pl.ds(x * WIDE * COLS, WIDE * COLS)],
                src.at[DEPTH + x],
            )
        fetch(own_ref.at[pl.ds(OWN_B, PLANES * 32)], stage.at[pl.ds(0, 128)])
        for s, (close, far) in enumerate(((pair_ref, even_ref), (cross_ref, odd_ref))):
            base = 0
            for d in range(1, PLANES + 1):
                count = (WIDE - 2 * d) * COLS
                fetch(close.at[pl.ds(base, count)], src.at[ghost(s, d), pl.ds(d * COLS, count)])
                base += count
            fetch(far.at[pl.ds(0, FAR_B)], src.at[ghost(s, DEPTH), pl.ds(DEPTH * COLS, FAR_B)])
            fetch(close.at[pl.ds(SEND_B, SEND_E)], stage.at[pl.ds(128 + s * 112, SEND_E)])
            fetch(far.at[pl.ds(FAR_B, ROWS)], stage.at[pl.ds(128 + s * 112 + 96, ROWS)])
        edge[...] = jnp.zeros_like(edge)
        part_ref[...] = jnp.zeros_like(part_ref)
        apart = lax.broadcasted_iota(jnp.int32, (LANES, LANES), 0) - lax.broadcasted_iota(
            jnp.int32, (LANES, LANES), 1
        )
        ones = jnp.where(jnp.abs(apart) == 1, 1.0, 0.0).astype(BF16)
        near[0:LANES, :] = ones
        near[LANES : 2 * LANES, :] = ones
        for c in copies:
            c.wait()
        for x in range(PLANES):
            edge[DEPTH + x] = stage[pl.ds(x * 32, 32), :]
        for s in range(2):
            for d in range(1, DEPTH + 1):
                edge[ghost(s, d), pl.ds(d, WIDE - 2 * d), :] = stage[
                    pl.ds(128 + s * 112 + (d - 1) * 24, WIDE - 2 * d), :
                ]

    def leaving(node):
        return [
            pltpu.make_async_copy(
                cat.at[pl.ds(64 * i, 64)],
                full_ref.at[pl.ds(pl.multiple_of(64 * node + 64 * i, 8), 64)],
                out_sem.at[i],
            )
            for i in range(1)
        ]

    start()

    @pl.loop(0, QUAD)
    def _(node):
        count = count_ref[node]
        freq = freq_ref[node]

        for px in range(SPAN):
            d = edge[px]
            inv = 1.0 / (d * d + freq * freq)
            gre[px] = d * inv
            gim[px] = jnp.where(d > 0.0, -freq * inv, 0.0)

        def planes(level, top, m, body):
            dd = level - m
            idle = (dd < 0) | (level > top)
            trips = jnp.where(idle, 0, jnp.where(dd == 0, PLANES // 2, 1))

            @pl.loop(0, trips)
            def _(q):
                left = jnp.where(dd == 0, DEPTH + 2 * q, DEPTH - dd)
                right = jnp.where(dd == 0, left + 1, DEPTH + PLANES - 1 + dd)
                body(left, right)

        def spread(ref, px, r):
            return jnp.broadcast_to(ref[px, pl.ds(r, 1), :], (COLS, LANES))

        def at_row(r):
            return pl.ds(r * COLS, COLS)

        def halves(v):
            hi = v.astype(BF16)
            return hi, (v - hi.astype(F32)).astype(BF16)

        def begin(field):
            for m in range(DEPTH + 1):

                def first(*pair_of, m=m):
                    for px in pair_of:
                        for r in range(DEPTH - m, DEPTH + ROWS + m):
                            b = src[px, at_row(r), :]
                            field[0, px, at_row(r), :] = spread(gre, px, r) * b
                            field[1, px, at_row(r), :] = spread(gim, px, r) * b

                planes(count - 1, count - 1, m, first)

        def sweep(old, emit, group, m):
            start, rows = DEPTH - m, ROWS + 2 * m
            beside = []
            for px in group:
                lhs = []
                for i in range(rows):
                    for c in range(2):
                        hi, lo = halves(old[c, px, at_row(start + i), :])
                        lhs.append(jnp.concatenate([hi, lo], 1))
                beside.append(
                    jnp.dot(jnp.concatenate(lhs, 0), near[...], preferred_element_type=F32)
                )
            for px, side in zip(group, beside):

                def get(c, p, r):
                    return old[c, p, at_row(r), :]

                below = [get(c, px, start - 1) for c in range(2)]
                here = [get(c, px, start) for c in range(2)]
                for i in range(rows):
                    r = start + i
                    above = [get(c, px, r + 1) for c in range(2)]
                    re, im = [
                        (get(c, px - 1, r) + get(c, px + 1, r))
                        + (below[c] + above[c])
                        + side[i * 32 + c * COLS : i * 32 + c * COLS + COLS]
                        for c in range(2)
                    ]
                    re = re + src[px, at_row(r), :]
                    p, q = spread(gre, px, r), spread(gim, px, r)
                    emit(px, r, (p * re - q * im, p * im + q * re))
                    below, here = here, above

        @pl.when(lax.rem(count, 2) == 1)
        def _():
            begin(even)

        @pl.when(lax.rem(count, 2) == 0)
        def _():
            begin(odd)

        def into(new):
            def emit(px, r, values):
                for c, v in enumerate(values):
                    new[c, px, at_row(r), :] = v

            return emit

        for level in range(DEPTH - 1, 0, -1):

            @pl.when(level <= count - 2)
            def _(level=level):
                old, new = (odd, even) if level % 2 == 0 else (even, odd)
                sweep(old, into(new), range(DEPTH, DEPTH + PLANES), level)
                for d in range(1, level + 1):
                    sweep(old, into(new), (DEPTH - d, DEPTH + PLANES - 1 + d), level - d)

        leave = leaving(node)

        @pl.when(node > 0)
        def _():
            for c in leave:
                c.wait()

        def finish(px, r, values):
            at = pl.ds(((px - DEPTH) * ROWS + r - DEPTH) * LANES, LANES)
            for c, v in enumerate(values):
                hi, lo = halves(v)
                cat[pl.ds(32 + c * COLS, COLS), at] = hi
                cat[pl.ds(c * COLS, COLS), at] = lo

        sweep(odd, finish, range(DEPTH, DEPTH + PLANES), 0)
        for c in leave:
            c.start()
        o = lax.dot_general(
            cat[32:96, :], cat[0:64, :], (((1,), (1,)), ((), ())), preferred_element_type=F32
        )
        o = jnp.concatenate([o, jnp.zeros((64, 64), F32)], 1)
        lane = lax.broadcasted_iota(jnp.int32, (COLS, LANES), 1)
        seen = o[32:48] + o[48:64]
        proj = seen + pltpu.roll(seen, LANES - 32, 1)
        proj = pltpu.roll(jnp.where(lane < 32, proj, 0.0), 32 * lax.rem(node, 4), 1)
        part_ref[pl.ds(pl.multiple_of(16 * (node // 4), 16), 16), :] += proj
        half = o[0:32] + 0.5 * pltpu.roll(o[0:32], LANES - 32, 1)
        gram = half[0:16] + pltpu.roll(half[16:32], LANES - 16, 1)
        gram = jnp.where(lane < 16, gram, 0.0)
        part_ref[32:48, :] += pltpu.roll(gram, 16 * node, 1)

    for c in leaving(0):
        c.wait()


def solve(at, freqs, counts, own, pair, cross, even, odd, probe):
    cells = PLANES * ROWS * LANES
    return pl.pallas_call(
        solve_kernel,
        out_shape=(
            jax.ShapeDtypeStruct((QUAD * 64, cells), BF16),
            jax.ShapeDtypeStruct((48, LANES), F32),
        ),
        in_specs=[SMEM, SMEM, SMEM] + [ANY] * 6,
        out_specs=(
            pl.BlockSpec(memory_space=pltpu.HBM),
            VMEM,
        ),
        scratch_shapes=[
            pltpu.VMEM((SPAN, WIDE * COLS, LANES), F32),
            pltpu.VMEM((2, SPAN, WIDE * COLS, LANES), F32),
            pltpu.VMEM((2, SPAN, WIDE * COLS, LANES), F32),
            pltpu.VMEM((2 * LANES, LANES), BF16),
            pltpu.VMEM((SPAN, 32, LANES), F32),
            pltpu.VMEM((SPAN, 32, LANES), F32),
            pltpu.VMEM((SPAN, 32, LANES), F32),
            pltpu.VMEM((96, cells), BF16),
            pltpu.VMEM((352, LANES), F32),
            pltpu.SemaphoreType.DMA((24,)),
            pltpu.SemaphoreType.DMA((8,)),
        ],
        compiler_params=pltpu.CompilerParams(vmem_limit_bytes=SOLVE_LIMIT),
        name="solve",
    )(at, freqs, counts, own, pair, cross, even, odd, probe)


def respond_kernel(pick_ref, weight_ref, sum_ref, full_ref, out_ref, gram_ref, coef, full, sems):
    parts = PLANES * ROWS // STEP
    wide = STEP * LANES
    copies = [
        [
            pltpu.make_async_copy(
                full_ref.at[pl.ds(128 * j, 128), pl.ds(t * wide, wide)],
                full.at[t, pl.ds(128 * j, 128), :],
                sems.at[t, j],
            )
            for j in range(4)
        ]
        for t in range(parts)
    ]
    for group in copies:
        for c in group:
            c.start()
    lane = lax.broadcasted_iota(jnp.int32, (16, LANES), 1)
    for half in range(2):
        scale = weight_ref[half * 4] * (1.0 / QUAD)
        for j in range(1, 4):
            scale = jnp.where(lane < 32 * j, scale, weight_ref[half * 4 + j] * (1.0 / QUAD))
        acc = sum_ref[16 * half : 16 * half + 16, :] * scale
        for b in range(2):
            one = pltpu.roll(acc, 64, 1) if b else acc
            twice = jnp.where(
                lane < 32,
                one,
                jnp.where(lane < 96, pltpu.roll(one, 32, 1), pltpu.roll(one, 64, 1)),
            )
            at = pl.ds((half * 2 + b) * LANES, LANES)
            hi = twice.astype(BF16)
            coef[0:16, at] = hi
            coef[16:32, at] = (twice - hi.astype(F32)).astype(BF16)
    node = pick_ref[0]
    gram = pltpu.roll(sum_ref[32:48, :], lax.rem(128 - 16 * node, 128), 1)
    gram = gram * (weight_ref[node] * (1.0 / CELLS))
    gram_ref[:, 0:16] = gram[:, 0:16] + gram.T[0:16, :]

    flat = out_ref.reshape(16 * PLANES * ROWS, LANES)
    for t, group in enumerate(copies):
        for c in group:
            c.wait()
        big = jnp.dot(coef[...], full[t], preferred_element_type=F32)
        res = big[0:16] + big[16:32]
        for y in range(STEP):
            flat[pl.ds(t * STEP + y, 16, stride=PLANES * ROWS), :] = res[
                :, y * LANES : (y + 1) * LANES
            ]


def respond(pick, weights, total, full):
    parts = PLANES * ROWS // STEP
    return pl.pallas_call(
        respond_kernel,
        out_shape=(
            jax.ShapeDtypeStruct((16, PLANES, ROWS, LANES), F32),
            jax.ShapeDtypeStruct((16, LANES), F32),
        ),
        in_specs=[SMEM, SMEM, VMEM, ANY],
        out_specs=(VMEM, VMEM),
        scratch_shapes=[
            pltpu.VMEM((32, QUAD * 64), BF16),
            pltpu.VMEM((parts, QUAD * 64, STEP * LANES), BF16),
            pltpu.SemaphoreType.DMA((parts, 4)),
        ],
        compiler_params=pltpu.CompilerParams(vmem_limit_bytes=50 << 20),
        name="respond",
    )(pick, weights, total, full)


def both_ways(pairs):
    return pairs + [(b, a) for a, b in pairs]


def swap_core(v):
    return lax.ppermute(v, "row", [(r, r ^ 1) for r in range(16)])


def swap_rows(v, step, chosen):
    pairs = []
    for node in range(8):
        for r in range(16 - step):
            if chosen(r):
                other = node ^ 4 if (r // 2) % 2 else node
                pairs.append((node * 16 + r, other * 16 + r + step))
    return lax.ppermute(v, ("node", "row"), both_ways(pairs))


def xor_sum(x, axis, size, masks):
    combos = [0]
    for m in masks:
        combos += [c ^ m for c in combos]
    got = [x if c == 0 else lax.ppermute(x, axis, [(i, i ^ c) for i in range(size)]) for c in combos]
    while len(got) > 1:
        got = [got[i] + got[i + 1] for i in range(0, len(got), 2)]
    return got[0]


def turn(v, mask):
    return lax.ppermute(v, "node", [(i, i ^ mask) for i in range(8)])


def across(v):
    return lax.ppermute(v, "node", [(i, i ^ 4) for i in range(8)])


def place_into(out_ref, spot_ref, pieces, spots, sems):
    copies = []
    for piece, (slot, first) in zip(pieces, spots):
        at = pl.multiple_of(spot_ref[slot], ROWS)
        for i in range(0, piece.shape[0], 4):
            dst = out_ref.at[pl.ds(first + i, 4), :, pl.ds(at, ROWS), :]
            copies.append(pltpu.make_async_copy(piece.at[pl.ds(i, 4)], dst, sems.at[len(copies)]))
    for c in copies:
        c.start()
    for c in copies:
        c.wait()


EARLY = ((0, 0), (1, 0), (2, 0), (4, 0), (3, 0), (3, 8))
LATE = ((5, 0), (6, 0), (7, 0), (7, 8))


def early_kernel(spot_ref, *refs):
    place_into(refs[6], spot_ref, refs[:6], EARLY, refs[7])


def late_kernel(spot_ref, *refs):
    place_into(refs[5], spot_ref, refs[:4], LATE, refs[6])


def place(spots, early, late):
    whole = jax.ShapeDtypeStruct((16, PLANES, 128, LANES), F32)
    params = pltpu.CompilerParams(vmem_limit_bytes=50 << 20)
    begun = pl.pallas_call(
        early_kernel,
        out_shape=whole,
        in_specs=[SMEM] + [VMEM] * 6,
        out_specs=ANY,
        scratch_shapes=[pltpu.SemaphoreType.DMA((20,))],
        compiler_params=params,
        name="early",
    )(spots, *early)
    return pl.pallas_call(
        late_kernel,
        out_shape=whole,
        in_specs=[SMEM] + [VMEM] * 4 + [ANY],
        out_specs=ANY,
        scratch_shapes=[pltpu.SemaphoreType.DMA((12,))],
        input_output_aliases={5: 0},
        compiler_params=params,
        name="late",
    )(spots, *late, begun)


def local(inputs, diagonal, observations, frequencies, weights, counts, assignment):
    node = lax.axis_index("node")
    row = lax.axis_index("row")
    core, odd = row % 2, (row // 2) % 2
    other = jnp.where(core == odd, node ^ 4, node)
    at = jnp.stack([16 * node, 16 * other, core, odd]).astype(jnp.int32)
    s1, s2, s3, s4 = pack(at, inputs, diagonal)
    own, probe = prep(at, inputs, diagonal, observations, s3)
    cross = swap_rows(s2, 1, lambda r: r % 2 == 1)
    far_even = swap_rows(s3, 2, lambda r: (r // 2) % 2 == 0)
    far_odd = swap_rows(s4, 2, lambda r: (r // 2) % 2 == 1)
    pair = swap_core(s1)
    fields, part = solve(at, frequencies, counts, own, pair, cross, far_even, far_odd, probe)
    total = xor_sum(part, "row", 16, [1, 2])
    total = xor_sum(total, "row", 16, [4, 8])
    total = xor_sum(total, "node", 8, [1, 2])
    total = xor_sum(total, "node", 8, [4])
    pick = lax.dynamic_slice_in_dim(assignment, node, 1)
    mine, gram = respond(pick, weights, total, fields)

    left, right, other = turn(mine, 1), turn(mine, 3), across(mine)
    far0, far1 = turn(right[:8], 1), turn(left[8:], 3)
    left_o, right_o = turn(other, 1), turn(other, 3)
    far0_o, far1_o = across(far0), across(far1)
    x, z = node % 4, node // 4
    spots = []
    for side in (z, 1 - z):
        spots += [(side * 4 + (x ^ mask)) * ROWS for mask in (0, 1, 3, 2)]
    full = place(
        jnp.stack(spots).astype(jnp.int32),
        (mine, left, right, other, far0, far1),
        (left_o, right_o, far0_o, far1_o),
    )
    return full, gram[None, :, :16]


def solution(mesh):
    placed = (
        P(None, "row", None, None),
        P("row", None, None),
        P(None, "row", None, None),
        P(),
        P(),
        P(),
        P(),
    )
    return jax.shard_map(
        local,
        mesh=mesh,
        in_specs=placed,
        out_specs=(P(None, "row", None, None), P("node", None, None)),
        check_vma=False,
    )
```

```python
import jax
import jax.numpy as jnp
from jax import lax
from jax.experimental import pallas as pl
from jax.experimental.pallas import tpu as pltpu
from jax.sharding import PartitionSpec as P

QUAD = 8
COLS = 16
DEPTH = 5
PLANES = 4
ROWS = 16
WIDE = ROWS + 2 * DEPTH
SPAN = PLANES + 2 * DEPTH
LANES = 128
CELLS = 1048576.0
SEND_B = sum(WIDE - 2 * d for d in range(1, PLANES + 1)) * COLS
SEND_E = PLANES * 24
FAR_B = ROWS * COLS
OWN_B = PLANES * WIDE * COLS
STEP = 8
PACK_LIMIT = 50 << 20
SOLVE_LIMIT = 51 << 20
F32 = jnp.float32
BF16 = jnp.bfloat16
VMEM = pl.BlockSpec(memory_space=pltpu.VMEM)
SMEM = pl.BlockSpec(memory_space=pltpu.SMEM)
ANY = pl.BlockSpec(memory_space=pl.ANY)


def window_copies(src_ref, start, dst_ref, sems):
    rows = pl.ds(pl.multiple_of(start, 8), 32)
    return [
        pltpu.make_async_copy(
            src_ref.at[pl.ds(2 * i, 2), :, rows, :], dst_ref.at[pl.ds(2 * i, 2)], sems.at[i]
        )
        for i in range(COLS // 2)
    ]


def first_row(at):
    return jnp.clip(at - 8, 0, 96)


def fill_edge(edge_ref, diag_ref):
    for x in range(PLANES):
        edge_ref[x, pl.ds(0, 16), :] = jnp.zeros((16, LANES), F32)
        edge_ref[x, pl.ds(144, 16), :] = jnp.zeros((16, LANES), F32)
        edge_ref[x, pl.ds(16, 128), :] = diag_ref[x] + 6.0


def turned_rows(dst_ref, base, flat_ref, offset, first, count):
    for q in range(count):
        y = jnp.clip(first + q, 0, 127) + offset
        dst_ref[pl.ds(base + q * COLS, COLS), :] = flat_ref[
            pl.ds(y, COLS, stride=PLANES * 32), :
        ]


def pack_kernel(
    at_ref, src_ref, diag_hbm, cross_ref, even_ref, odd_ref, edge_ref, diag_ref, win, sems
):
    mine = at_ref[0]
    other = jnp.where(mine >= 64, mine - 64, mine + 64)
    whole = pltpu.make_async_copy(diag_hbm, diag_ref, sems.at[2, 0])
    whole.start()
    copies = []
    for w, t in enumerate((mine, other)):
        copies += window_copies(src_ref, first_row(t), win.at[w], sems.at[w])
    for c in copies:
        c.start()
    whole.wait()
    fill_edge(edge_ref, diag_ref)
    for c in copies:
        c.wait()
    flat = win.reshape(2 * COLS * PLANES * 32, LANES)

    def send(dst_ref, base, at, plane, d, count):
        offset = jnp.where(at == mine, 0, COLS * PLANES * 32) + plane * 32 - first_row(at)
        turned_rows(dst_ref, base, flat, offset, at - DEPTH + d, count)

    core, odd = at_ref[2], at_ref[3]
    base = 0
    for d in range(1, PLANES + 1):
        count = WIDE - 2 * d
        at = at_ref[1]
        plane = jnp.where(core == 1, PLANES - d, d - 1)
        send(cross_ref, base, at, plane, d, count)
        cross_ref[pl.ds(SEND_B + (d - 1) * 24, 24), :] = edge_ref[
            plane, pl.ds(16 + at - DEPTH + d, 24), :
        ]
        base += count * COLS
    for dst_ref, at, right in ((even_ref, mine, odd == 0), (odd_ref, other, odd == 1)):
        plane = jnp.where(right, PLANES - 1, 0)
        send(dst_ref, 0, at, plane, DEPTH, ROWS)
        dst_ref[pl.ds(FAR_B, ROWS), :] = edge_ref[plane, pl.ds(16 + at, ROWS), :]


def pack(at, inputs, diagonal):
    out = lambda n: jax.ShapeDtypeStruct((n, LANES), F32)
    return pl.pallas_call(
        pack_kernel,
        out_shape=(
            out(SEND_B + SEND_E),
            out(FAR_B + ROWS),
            out(FAR_B + ROWS),
        ),
        in_specs=[SMEM, ANY, ANY],
        out_specs=(VMEM,) * 3,
        scratch_shapes=[
            pltpu.VMEM((PLANES, 160, LANES), F32),
            pltpu.VMEM((PLANES, 128, LANES), F32),
            pltpu.VMEM((2, COLS, PLANES, 32, LANES), F32),
            pltpu.SemaphoreType.DMA((3, 8)),
        ],
        compiler_params=pltpu.CompilerParams(vmem_limit_bytes=PACK_LIMIT),
        name="pack",
    )(at, inputs, diagonal)


def prep_kernel(
    at_ref, src_ref, diag_ref, obs_ref, after_ref, own_ref, probe_ref, pair_ref, edge_ref, win, obs, sems
):
    mine = at_ref[0]
    copies = window_copies(src_ref, first_row(mine), win, sems)
    copies.append(
        pltpu.make_async_copy(
            obs_ref.at[:, :, pl.ds(pl.multiple_of(mine, 16), ROWS), :], obs, sems.at[8]
        )
    )
    for c in copies:
        c.start()
    fill_edge(edge_ref, diag_ref)
    for c in copies:
        c.wait()
    flat = win.reshape(COLS * PLANES * 32, LANES)
    seen = obs.reshape(COLS * PLANES * ROWS, LANES)
    base = 0
    for d in range(1, PLANES + 1):
        count = WIDE - 2 * d
        plane = jnp.where(at_ref[2] == 0, PLANES - d, d - 1)
        turned_rows(
            pair_ref, base, flat, plane * 32 - first_row(mine), mine - DEPTH + d, count
        )
        pair_ref[pl.ds(SEND_B + (d - 1) * 24, 24), :] = edge_ref[
            plane, pl.ds(16 + mine - DEPTH + d, 24), :
        ]
        base += count * COLS
    for x in range(PLANES):
        offset = x * 32 - first_row(mine)
        turned_rows(own_ref, x * WIDE * COLS, flat, offset, mine - DEPTH, WIDE)
        own_ref[pl.ds(OWN_B + x * 32, 32), :] = edge_ref[x, pl.ds(16 + mine - DEPTH, 32), :]
        for y in range(ROWS):
            v = seen[pl.ds(x * ROWS + y, COLS, stride=PLANES * ROWS), :]
            hi = v.astype(BF16)
            at = pl.ds((x * ROWS + y) * LANES, LANES)
            probe_ref[0:16, at] = hi
            probe_ref[16:32, at] = (v - hi.astype(F32)).astype(BF16)


def prep(at, inputs, diagonal, observations, after):
    return pl.pallas_call(
        prep_kernel,
        out_shape=(
            jax.ShapeDtypeStruct((OWN_B + PLANES * 32, LANES), F32),
            jax.ShapeDtypeStruct((32, PLANES * ROWS * LANES), BF16),
            jax.ShapeDtypeStruct((SEND_B + SEND_E, LANES), F32),
        ),
        in_specs=[SMEM, ANY, VMEM, ANY, ANY],
        out_specs=(VMEM, VMEM, VMEM),
        scratch_shapes=[
            pltpu.VMEM((PLANES, 160, LANES), F32),
            pltpu.VMEM((COLS, PLANES, 32, LANES), F32),
            pltpu.VMEM((COLS, PLANES, ROWS, LANES), F32),
            pltpu.SemaphoreType.DMA((9,)),
        ],
        compiler_params=pltpu.CompilerParams(vmem_limit_bytes=PACK_LIMIT),
        cost_estimate=pl.CostEstimate(flops=40_000_000, bytes_accessed=4_000_000, transcendentals=0),
        name="prep",
    )(at, inputs, diagonal, observations, after)


def solve_kernel(
    at_ref, freq_ref, count_ref, own_ref, pair_ref, cross_ref, even_ref, odd_ref, probe_ref,
    full_ref, part_ref,
    src, even, odd, near, edge, gre, gim, cat, stage, sems, out_sem,
):
    core, half_odd = at_ref[2], at_ref[3]

    def ghost(s, d):
        if d < DEPTH:
            right = core == s
        else:
            right = half_odd == s
        return jnp.where(right, DEPTH + PLANES - 1 + d, DEPTH - d)

    def start():
        copies = []

        def fetch(a, b):
            copies.append(pltpu.make_async_copy(a, b, sems.at[len(copies)]))
            copies[-1].start()

        fetch(probe_ref, cat.at[pl.ds(64, 32)])
        for x in range(PLANES):
            fetch(
                own_ref.at[pl.ds(x * WIDE * COLS, WIDE * COLS)],
                src.at[DEPTH + x],
            )
        fetch(own_ref.at[pl.ds(OWN_B, PLANES * 32)], stage.at[pl.ds(0, 128)])
        for s, (close, far) in enumerate(((pair_ref, even_ref), (cross_ref, odd_ref))):
            base = 0
            for d in range(1, PLANES + 1):
                count = (WIDE - 2 * d) * COLS
                fetch(close.at[pl.ds(base, count)], src.at[ghost(s, d), pl.ds(d * COLS, count)])
                base += count
            fetch(far.at[pl.ds(0, FAR_B)], src.at[ghost(s, DEPTH), pl.ds(DEPTH * COLS, FAR_B)])
            fetch(close.at[pl.ds(SEND_B, SEND_E)], stage.at[pl.ds(128 + s * 112, SEND_E)])
            fetch(far.at[pl.ds(FAR_B, ROWS)], stage.at[pl.ds(128 + s * 112 + 96, ROWS)])
        edge[...] = jnp.zeros_like(edge)
        part_ref[...] = jnp.zeros_like(part_ref)
        apart = lax.broadcasted_iota(jnp.int32, (LANES, LANES), 0) - lax.broadcasted_iota(
            jnp.int32, (LANES, LANES), 1
        )
        ones = jnp.where(jnp.abs(apart) == 1, 1.0, 0.0).astype(BF16)
        near[0:LANES, :] = ones
        near[LANES : 2 * LANES, :] = ones
        for c in copies:
            c.wait()
        for x in range(PLANES):
            edge[DEPTH + x] = stage[pl.ds(x * 32, 32), :]
        for s in range(2):
            for d in range(1, DEPTH + 1):
                edge[ghost(s, d), pl.ds(d, WIDE - 2 * d), :] = stage[
                    pl.ds(128 + s * 112 + (d - 1) * 24, WIDE - 2 * d), :
                ]

    def leaving(node):
        return [
            pltpu.make_async_copy(
                cat.at[pl.ds(64 * i, 64)],
                full_ref.at[pl.ds(pl.multiple_of(64 * node + 64 * i, 8), 64)],
                out_sem.at[i],
            )
            for i in range(1)
        ]

    start()

    @pl.loop(0, QUAD)
    def _(node):
        count = count_ref[node]
        freq = freq_ref[node]

        for px in range(SPAN):
            d = edge[px]
            inv = 1.0 / (d * d + freq * freq)
            gre[px] = d * inv
            gim[px] = jnp.where(d > 0.0, -freq * inv, 0.0)

        def planes(level, top, m, body):
            dd = level - m
            idle = (dd < 0) | (level > top)
            trips = jnp.where(idle, 0, jnp.where(dd == 0, PLANES // 2, 1))

            @pl.loop(0, trips)
            def _(q):
                left = jnp.where(dd == 0, DEPTH + 2 * q, DEPTH - dd)
                right = jnp.where(dd == 0, left + 1, DEPTH + PLANES - 1 + dd)
                body(left, right)

        def spread(ref, px, r):
            return jnp.broadcast_to(ref[px, pl.ds(r, 1), :], (COLS, LANES))

        def at_row(r):
            return pl.ds(r * COLS, COLS)

        def halves(v):
            hi = v.astype(BF16)
            return hi, (v - hi.astype(F32)).astype(BF16)

        def begin(field):
            for m in range(DEPTH + 1):

                def first(*pair_of, m=m):
                    for px in pair_of:
                        for r in range(DEPTH - m, DEPTH + ROWS + m):
                            b = src[px, at_row(r), :]
                            field[0, px, at_row(r), :] = spread(gre, px, r) * b
                            field[1, px, at_row(r), :] = spread(gim, px, r) * b

                planes(count - 1, count - 1, m, first)

        def sweep(old, emit, group, m):
            start, rows = DEPTH - m, ROWS + 2 * m
            beside = []
            for px in group:
                lhs = []
                for i in range(rows):
                    for c in range(2):
                        hi, lo = halves(old[c, px, at_row(start + i), :])
                        lhs.append(jnp.concatenate([hi, lo], 1))
                beside.append(
                    jnp.dot(jnp.concatenate(lhs, 0), near[...], preferred_element_type=F32)
                )
            for px, side in zip(group, beside):

                def get(c, p, r):
                    return old[c, p, at_row(r), :]

                below = [get(c, px, start - 1) for c in range(2)]
                here = [get(c, px, start) for c in range(2)]
                for i in range(rows):
                    r = start + i
                    above = [get(c, px, r + 1) for c in range(2)]
                    re, im = [
                        (get(c, px - 1, r) + get(c, px + 1, r))
                        + (below[c] + above[c])
                        + side[i * 32 + c * COLS : i * 32 + c * COLS + COLS]
                        for c in range(2)
                    ]
                    re = re + src[px, at_row(r), :]
                    p, q = spread(gre, px, r), spread(gim, px, r)
                    emit(px, r, (p * re - q * im, p * im + q * re))
                    below, here = here, above

        @pl.when(lax.rem(count, 2) == 1)
        def _():
            begin(even)

        @pl.when(lax.rem(count, 2) == 0)
        def _():
            begin(odd)

        def into(new):
            def emit(px, r, values):
                for c, v in enumerate(values):
                    new[c, px, at_row(r), :] = v

            return emit

        for level in range(DEPTH - 1, 0, -1):

            @pl.when(level <= count - 2)
            def _(level=level):
                old, new = (odd, even) if level % 2 == 0 else (even, odd)
                sweep(old, into(new), range(DEPTH, DEPTH + PLANES), level)
                for d in range(1, level + 1):
                    sweep(old, into(new), (DEPTH - d, DEPTH + PLANES - 1 + d), level - d)

        leave = leaving(node)

        @pl.when(node > 0)
        def _():
            for c in leave:
                c.wait()

        def finish(px, r, values):
            at = pl.ds(((px - DEPTH) * ROWS + r - DEPTH) * LANES, LANES)
            for c, v in enumerate(values):
                hi, lo = halves(v)
                cat[pl.ds(32 + c * COLS, COLS), at] = hi
                cat[pl.ds(c * COLS, COLS), at] = lo

        sweep(odd, finish, range(DEPTH, DEPTH + PLANES), 0)
        for c in leave:
            c.start()
        o = lax.dot_general(
            cat[32:96, :], cat[0:64, :], (((1,), (1,)), ((), ())), preferred_element_type=F32
        )
        o = jnp.concatenate([o, jnp.zeros((64, 64), F32)], 1)
        lane = lax.broadcasted_iota(jnp.int32, (COLS, LANES), 1)
        seen = o[32:48] + o[48:64]
        proj = seen + pltpu.roll(seen, LANES - 32, 1)
        proj = pltpu.roll(jnp.where(lane < 32, proj, 0.0), 32 * lax.rem(node, 4), 1)
        part_ref[pl.ds(pl.multiple_of(16 * (node // 4), 16), 16), :] += proj
        half = o[0:32] + 0.5 * pltpu.roll(o[0:32], LANES - 32, 1)
        gram = half[0:16] + pltpu.roll(half[16:32], LANES - 16, 1)
        gram = jnp.where(lane < 16, gram, 0.0)
        part_ref[32:48, :] += pltpu.roll(gram, 16 * node, 1)

    for c in leaving(0):
        c.wait()


def solve(at, freqs, counts, own, pair, cross, even, odd, probe):
    cells = PLANES * ROWS * LANES
    return pl.pallas_call(
        solve_kernel,
        out_shape=(
            jax.ShapeDtypeStruct((QUAD * 64, cells), BF16),
            jax.ShapeDtypeStruct((48, LANES), F32),
        ),
        in_specs=[SMEM, SMEM, SMEM] + [ANY] * 6,
        out_specs=(
            pl.BlockSpec(memory_space=pltpu.HBM),
            VMEM,
        ),
        scratch_shapes=[
            pltpu.VMEM((SPAN, WIDE * COLS, LANES), F32),
            pltpu.VMEM((2, SPAN, WIDE * COLS, LANES), F32),
            pltpu.VMEM((2, SPAN, WIDE * COLS, LANES), F32),
            pltpu.VMEM((2 * LANES, LANES), BF16),
            pltpu.VMEM((SPAN, 32, LANES), F32),
            pltpu.VMEM((SPAN, 32, LANES), F32),
            pltpu.VMEM((SPAN, 32, LANES), F32),
            pltpu.VMEM((96, cells), BF16),
            pltpu.VMEM((352, LANES), F32),
            pltpu.SemaphoreType.DMA((24,)),
            pltpu.SemaphoreType.DMA((8,)),
        ],
        compiler_params=pltpu.CompilerParams(vmem_limit_bytes=SOLVE_LIMIT),
        name="solve",
    )(at, freqs, counts, own, pair, cross, even, odd, probe)


def respond_kernel(pick_ref, weight_ref, sum_ref, full_ref, out_ref, gram_ref, coef, full, sems):
    parts = PLANES * ROWS // STEP
    wide = STEP * LANES
    copies = [
        [
            pltpu.make_async_copy(
                full_ref.at[pl.ds(128 * j, 128), pl.ds(t * wide, wide)],
                full.at[t, pl.ds(128 * j, 128), :],
                sems.at[t, j],
            )
            for j in range(4)
        ]
        for t in range(parts)
    ]
    for group in copies:
        for c in group:
            c.start()
    lane = lax.broadcasted_iota(jnp.int32, (16, LANES), 1)
    for half in range(2):
        scale = weight_ref[half * 4] * (1.0 / QUAD)
        for j in range(1, 4):
            scale = jnp.where(lane < 32 * j, scale, weight_ref[half * 4 + j] * (1.0 / QUAD))
        acc = sum_ref[16 * half : 16 * half + 16, :] * scale
        for b in range(2):
            one = pltpu.roll(acc, 64, 1) if b else acc
            twice = jnp.where(
                lane < 32,
                one,
                jnp.where(lane < 96, pltpu.roll(one, 32, 1), pltpu.roll(one, 64, 1)),
            )
            at = pl.ds((half * 2 + b) * LANES, LANES)
            hi = twice.astype(BF16)
            coef[0:16, at] = hi
            coef[16:32, at] = (twice - hi.astype(F32)).astype(BF16)
    node = pick_ref[0]
    gram = pltpu.roll(sum_ref[32:48, :], lax.rem(128 - 16 * node, 128), 1)
    gram = gram * (weight_ref[node] * (1.0 / CELLS))
    gram_ref[:, 0:16] = gram[:, 0:16] + gram.T[0:16, :]

    flat = out_ref.reshape(16 * PLANES * ROWS, LANES)
    for t, group in enumerate(copies):
        for c in group:
            c.wait()
        big = jnp.dot(coef[...], full[t], preferred_element_type=F32)
        res = big[0:16] + big[16:32]
        for y in range(STEP):
            flat[pl.ds(t * STEP + y, 16, stride=PLANES * ROWS), :] = res[
                :, y * LANES : (y + 1) * LANES
            ]


def respond(pick, weights, total, full):
    parts = PLANES * ROWS // STEP
    return pl.pallas_call(
        respond_kernel,
        out_shape=(
            jax.ShapeDtypeStruct((16, PLANES, ROWS, LANES), F32),
            jax.ShapeDtypeStruct((16, LANES), F32),
        ),
        in_specs=[SMEM, SMEM, VMEM, ANY],
        out_specs=(VMEM, VMEM),
        scratch_shapes=[
            pltpu.VMEM((32, QUAD * 64), BF16),
            pltpu.VMEM((parts, QUAD * 64, STEP * LANES), BF16),
            pltpu.SemaphoreType.DMA((parts, 4)),
        ],
        compiler_params=pltpu.CompilerParams(vmem_limit_bytes=50 << 20),
        name="respond",
    )(pick, weights, total, full)


def both_ways(pairs):
    return pairs + [(b, a) for a, b in pairs]


def swap_core(v):
    return lax.ppermute(v, "row", [(r, r ^ 1) for r in range(16)])


def swap_rows(v, step, chosen):
    pairs = []
    for node in range(8):
        for r in range(16 - step):
            if chosen(r):
                other = node ^ 4 if (r // 2) % 2 else node
                pairs.append((node * 16 + r, other * 16 + r + step))
    return lax.ppermute(v, ("node", "row"), both_ways(pairs))


def xor_sum(x, axis, size, masks):
    combos = [0]
    for m in masks:
        combos += [c ^ m for c in combos]
    got = [x if c == 0 else lax.ppermute(x, axis, [(i, i ^ c) for i in range(size)]) for c in combos]
    while len(got) > 1:
        got = [got[i] + got[i + 1] for i in range(0, len(got), 2)]
    return got[0]


def turn(v, mask):
    return lax.ppermute(v, "node", [(i, i ^ mask) for i in range(8)])


def across(v):
    return lax.ppermute(v, "node", [(i, i ^ 4) for i in range(8)])


def place_into(out_ref, spot_ref, pieces, spots, sems):
    copies = []
    for piece, (slot, first) in zip(pieces, spots):
        at = pl.multiple_of(spot_ref[slot], ROWS)
        for i in range(0, piece.shape[0], 4):
            dst = out_ref.at[pl.ds(first + i, 4), :, pl.ds(at, ROWS), :]
            copies.append(pltpu.make_async_copy(piece.at[pl.ds(i, 4)], dst, sems.at[len(copies)]))
    for c in copies:
        c.start()
    for c in copies:
        c.wait()


EARLY = ((0, 0), (1, 0), (2, 0), (4, 0), (3, 0), (3, 8))
LATE = ((5, 0), (6, 0), (7, 0), (7, 8))


def early_kernel(spot_ref, *refs):
    place_into(refs[6], spot_ref, refs[:6], EARLY, refs[7])


def late_kernel(spot_ref, *refs):
    place_into(refs[5], spot_ref, refs[:4], LATE, refs[6])


def place(spots, early, late):
    whole = jax.ShapeDtypeStruct((16, PLANES, 128, LANES), F32)
    params = pltpu.CompilerParams(vmem_limit_bytes=50 << 20)
    begun = pl.pallas_call(
        early_kernel,
        out_shape=whole,
        in_specs=[SMEM] + [VMEM] * 6,
        out_specs=ANY,
        scratch_shapes=[pltpu.SemaphoreType.DMA((20,))],
        compiler_params=params,
        name="early",
    )(spots, *early)
    return pl.pallas_call(
        late_kernel,
        out_shape=whole,
        in_specs=[SMEM] + [VMEM] * 4 + [ANY],
        out_specs=ANY,
        scratch_shapes=[pltpu.SemaphoreType.DMA((12,))],
        input_output_aliases={5: 0},
        compiler_params=params,
        name="late",
    )(spots, *late, begun)


def local(inputs, diagonal, observations, frequencies, weights, counts, assignment):
    node = lax.axis_index("node")
    row = lax.axis_index("row")
    core, odd = row % 2, (row // 2) % 2
    other = jnp.where(core == odd, node ^ 4, node)
    at = jnp.stack([16 * node, 16 * other, core, odd]).astype(jnp.int32)
    s2, s3, s4 = pack(at, inputs, diagonal)
    cross = swap_rows(s2, 1, lambda r: r % 2 == 1)
    far_even = swap_rows(s3, 2, lambda r: (r // 2) % 2 == 0)
    far_odd = swap_rows(s4, 2, lambda r: (r // 2) % 2 == 1)
    own, probe, s1 = prep(at, inputs, diagonal, observations, s3)
    pair = swap_core(s1)
    fields, part = solve(at, frequencies, counts, own, pair, cross, far_even, far_odd, probe)
    total = xor_sum(part, "row", 16, [1, 2])
    total = xor_sum(total, "row", 16, [4, 8])
    total = xor_sum(total, "node", 8, [1, 2])
    total = xor_sum(total, "node", 8, [4])
    pick = lax.dynamic_slice_in_dim(assignment, node, 1)
    mine, gram = respond(pick, weights, total, fields)

    left, right, other = turn(mine, 1), turn(mine, 3), across(mine)
    far0, far1 = turn(right[:8], 1), turn(left[8:], 3)
    left_o, right_o = turn(other, 1), turn(other, 3)
    far0_o, far1_o = across(far0), across(far1)
    x, z = node % 4, node // 4
    spots = []
    for side in (z, 1 - z):
        spots += [(side * 4 + (x ^ mask)) * ROWS for mask in (0, 1, 3, 2)]
    full = place(
        jnp.stack(spots).astype(jnp.int32),
        (mine, left, right, other, far0, far1),
        (left_o, right_o, far0_o, far1_o),
    )
    return full, gram[None, :, :16]


def solution(mesh):
    placed = (
        P(None, "row", None, None),
        P("row", None, None),
        P(None, "row", None, None),
        P(),
        P(),
        P(),
        P(),
    )
    return jax.shard_map(
        local,
        mesh=mesh,
        in_specs=placed,
        out_specs=(P(None, "row", None, None), P("node", None, None)),
        check_vma=False,
    )
```
